32 devices in a mesh: replica: 2 (over x), yz: 4 (over z), x: 4 (over y, core).
Axes of the slice: x: 2, y: 2, z: 4, core: 2. Of those that a mesh axis runs over, the one named last changes fastest.
Arguments:
- hidden: bfloat16 [256, 4096], P('replica', ('x', 'yz')), parts along dimension 0
- seq_lens: int32 [256], P(('replica', 'yz', 'x')), parts along dimension 0
- attn_gain: bfloat16 [1, 4096], replicated
- mlp_gain: bfloat16 [1, 4096], replicated
- w_qkv: bfloat16 [1, 4096, 4352], P(None, None, 'yz')
- w_out: bfloat16 [1, 4096, 4096], P(None, 'yz')
- w_gate_up: bfloat16 [1, 4096, 2, 14336], P(None, None, None, 'yz')
- w_down: bfloat16 [1, 14336, 4096], P(None, 'yz')
- k_cache: bfloat16 [1, 256, 4096, 128], P(None, ('replica', 'yz', 'x')), parts along dimension 1
- v_cache: bfloat16 [1, 256, 4096, 128], P(None, ('replica', 'yz', 'x')), parts along dimension 1
Outputs:
- output 1: bfloat16 [256, 4096], P('replica', ('x', 'yz')), parts along dimension 0
- output 2: bfloat16 [1, 256, 4096, 128], P(None, ('replica', 'yz', 'x')), parts along dimension 1
- output 3: bfloat16 [1, 256, 4096, 128], P(None, ('replica', 'yz', 'x')), parts along dimension 1
There are 2 independent parts. The reference program is written for one: setup_inputs(seed, part) draws one part's arguments, and reference() takes and returns one part's arrays. A program takes and returns all parts, laid end to end along the dimension named above; an argument that names none is the same for every part.
All inputs are finite; a program needn't handle non-finite values.
Results may differ from the reference program's by a relative error of at most 0.0139522.
Values are sent between devices in bfloat16 or wider.
A program may use at most 1 GiB of HBM per device.

```python
import jax
import jax.numpy as jnp
from jax import lax

MODEL_DIM = 4096
Q_HEADS = 32
HEAD_DIM = 128
FFN_DIM = 14336
LAYERS = 1
SEQ_LEN = 4096
PART_BATCH = 128
BLOCK_ROWS = 8
ATTN_WIDTH = Q_HEADS * HEAD_DIM
QKV_WIDTH = ATTN_WIDTH + 2 * HEAD_DIM
NORM_EPS = 1e-5


def setup_inputs(seed: int = 0, part: int = 0) -> dict:
    root_key = jax.random.key(seed)
    shared = jax.random.split(root_key, 6)
    own_keys = jax.random.split(jax.random.fold_in(root_key, part), 6)
    cache_shape = (LAYERS, PART_BATCH, SEQ_LEN, HEAD_DIM)
    profile = 0.3 + 1.7 * jnp.arange(MODEL_DIM, dtype=jnp.float32) / MODEL_DIM
    row_scale = jnp.exp(0.5 * jax.random.normal(own_keys[0], (PART_BATCH, 1), jnp.float32))
    hidden = jax.random.normal(own_keys[1], (PART_BATCH, MODEL_DIM), jnp.float32) * profile * row_scale
    seq_lens = jax.random.randint(own_keys[2], (PART_BATCH,), 1, SEQ_LEN, dtype=jnp.int32)
    seq_lens = seq_lens.at[0].set(SEQ_LEN - 1).at[1].set(1)
    attn_gain = 1.0 + 0.5 * jax.random.normal(shared[0], (LAYERS, MODEL_DIM), jnp.float32)
    mlp_gain = 1.0 + 0.5 * jax.random.normal(shared[1], (LAYERS, MODEL_DIM), jnp.float32)
    w_qkv = jax.random.normal(shared[2], (LAYERS, MODEL_DIM, QKV_WIDTH), jnp.float32) * MODEL_DIM ** -0.5
    w_out = jax.random.normal(shared[3], (LAYERS, ATTN_WIDTH, MODEL_DIM), jnp.float32) * ATTN_WIDTH ** -0.5
    w_gate_up = jax.random.normal(shared[4], (LAYERS, MODEL_DIM, 2, FFN_DIM), jnp.float32) * MODEL_DIM ** -0.5
    w_down = jax.random.normal(shared[5], (LAYERS, FFN_DIM, MODEL_DIM), jnp.float32) * FFN_DIM ** -0.5
    k_cache = 2.0 * jax.random.normal(own_keys[3], cache_shape, jnp.float32)
    rand_walk = jnp.cumsum(jax.random.normal(own_keys[4], cache_shape, jnp.float32), axis=2)
    v_cache = rand_walk * (2.0 / SEQ_LEN ** 0.5) + jax.random.normal(own_keys[5], cache_shape, jnp.float32)
    return {
        'hidden': hidden.astype(jnp.bfloat16),
        'seq_lens': seq_lens,
        'attn_gain': attn_gain.astype(jnp.bfloat16),
        'mlp_gain': mlp_gain.astype(jnp.bfloat16),
        'w_qkv': w_qkv.astype(jnp.bfloat16),
        'w_out': w_out.astype(jnp.bfloat16),
        'w_gate_up': w_gate_up.astype(jnp.bfloat16),
        'w_down': w_down.astype(jnp.bfloat16),
        'k_cache': k_cache.astype(jnp.bfloat16),
        'v_cache': v_cache.astype(jnp.bfloat16),
    }


def rms_bf16(hid_state, gain):
    hid_f = hid_state.astype(jnp.float32)
    inv_scale = lax.rsqrt(jnp.mean(hid_f * hid_f, axis=-1, keepdims=True) + NORM_EPS)
    return (hid_f * inv_scale * gain.astype(jnp.float32)).astype(jnp.bfloat16)


def attend_block(row_block):
    z_rows, k_layer, v_layer, lens_blk = row_block
    queries = z_rows[:, :ATTN_WIDTH].reshape(BLOCK_ROWS, Q_HEADS, HEAD_DIM)
    k_new = z_rows[:, ATTN_WIDTH:ATTN_WIDTH + HEAD_DIM]
    v_new = z_rows[:, ATTN_WIDTH + HEAD_DIM:]
    slot_ids = jnp.arange(SEQ_LEN)
    at_slot = (slot_ids[None, :] == lens_blk[:, None])[:, :, None]
    k_upd = jnp.where(at_slot, k_new[:, None, :], k_layer)
    v_upd = jnp.where(at_slot, v_new[:, None, :], v_layer)
    scores = jnp.einsum('bhd,bsd->bhs', queries.astype(jnp.float32), k_upd.astype(jnp.float32)) * HEAD_DIM ** -0.5
    visible = (slot_ids[None, :] <= lens_blk[:, None])[:, None, :]
    scores = jnp.where(visible, scores, -1e30)
    probs_bf = jax.nn.softmax(scores, axis=-1).astype(jnp.bfloat16)
    outputs = jnp.einsum('bhs,bsd->bhd', probs_bf.astype(jnp.float32), v_upd.astype(jnp.float32)).astype(jnp.bfloat16)
    return outputs.reshape(BLOCK_ROWS, ATTN_WIDTH), k_upd, v_upd


def reference(hidden, seq_lens, attn_gain, mlp_gain, w_qkv, w_out, w_gate_up, w_down, k_cache, v_cache):
    num_blocks = PART_BATCH // BLOCK_ROWS

    def layer_step(hid_state, per_layer):
        gain_attn, gain_mlp, layer_qkv, layer_out, layer_gu, layer_down, k_layer, v_layer = per_layer
        normed = rms_bf16(hid_state, gain_attn)
        z_rows = jnp.dot(normed, layer_qkv, preferred_element_type=jnp.float32).astype(jnp.bfloat16)
        attn_out, k_upd, v_upd = lax.map(attend_block, (
            z_rows.reshape(num_blocks, BLOCK_ROWS, QKV_WIDTH),
            k_layer.reshape(num_blocks, BLOCK_ROWS, SEQ_LEN, HEAD_DIM),
            v_layer.reshape(num_blocks, BLOCK_ROWS, SEQ_LEN, HEAD_DIM),
            seq_lens.reshape(num_blocks, BLOCK_ROWS)))
        attn_out = attn_out.reshape(PART_BATCH, ATTN_WIDTH)
        hid_state = (hid_state.astype(jnp.float32) + jnp.dot(attn_out, layer_out, preferred_element_type=jnp.float32)).astype(jnp.bfloat16)
        normed = rms_bf16(hid_state, gain_mlp)
        gate_up = jnp.dot(normed, layer_gu.reshape(MODEL_DIM, 2 * FFN_DIM), preferred_element_type=jnp.float32).astype(jnp.bfloat16)
        gate_val = gate_up[:, :FFN_DIM].astype(jnp.float32)
        up_val = gate_up[:, FFN_DIM:].astype(jnp.float32)
        mlp_mixed = (jax.nn.silu(gate_val) * up_val).astype(jnp.bfloat16)
        hid_state = (hid_state.astype(jnp.float32) + jnp.dot(mlp_mixed, layer_down, preferred_element_type=jnp.float32)).astype(jnp.bfloat16)
        return hid_state, (k_upd.reshape(PART_BATCH, SEQ_LEN, HEAD_DIM), v_upd.reshape(PART_BATCH, SEQ_LEN, HEAD_DIM))

    hidden_out, caches = lax.scan(layer_step, hidden, (attn_gain, mlp_gain, w_qkv, w_out, w_gate_up, w_down, k_cache, v_cache))
    return hidden_out, caches[0], caches[1]
```

```python
import functools

import jax
import jax.numpy as jnp
from jax import lax
from jax.experimental import pallas as pl
from jax.experimental.pallas import tpu as pltpu
from jax.sharding import PartitionSpec as P

NORM_EPS = 1e-5
MESH = pl.DeviceIdType.MESH
BF = jnp.bfloat16
F32 = jnp.float32
MIB = 1024 * 1024


def at(z, x):
    return {"yz": z, "x": x}


def remote(src, dst, ssem, rsem, z, x):
    return pltpu.make_async_remote_copy(src_ref=src, dst_ref=dst, send_sem=ssem, recv_sem=rsem,
                                        device_id=at(z, x), device_id_type=MESH)


def group_barrier(z, x):
    sem = pltpu.get_barrier_semaphore()
    me = z * 4 + x

    def body(p, c):
        d = lax.rem(me + p, 16)
        pl.semaphore_signal(sem, inc=1, device_id=at(lax.div(d, 4), lax.rem(d, 4)), device_id_type=MESH)
        return c

    lax.fori_loop(1, 16, body, 0)
    pl.semaphore_wait(sem, 15)


def by_distance(z):
    a, b = lax.div(z, 2), lax.rem(z, 2)
    first = lax.div(z + 3, 4)
    n1 = first * (z - 1) + (1 - first)
    n2 = 2 + a * (1 - 2 * b)
    return n1, n2, 6 - z - n1 - n2


def gather(buf, slot, src_for, ssem, rsem, z, x):
    yx = lax.rem(x + 2, 4)
    cx = x + 1 - 2 * lax.rem(x, 2)
    cyx = lax.rem(cx + 2, 4)
    near = by_distance(z)
    me = slot(z, x)
    started = []

    def send(src, s, zt, xt):
        cp = remote(src, buf.at[s], ssem.at[len(started)], rsem.at[s], zt, xt)
        cp.start()
        started.append(cp)

    def arrived(s):
        remote(buf.at[s], buf.at[s], ssem.at[0], rsem.at[s], z, x).wait_recv()

    send(src_for(z), me, z, yx)
    for zt in near:
        send(src_for(zt), me, zt, x)
    send(src_for(z), me, z, cx)
    s = slot(z, yx)
    arrived(s)
    send(buf.at[s], s, z, cx)
    for zt in near:
        s = slot(zt, x)
        arrived(s)
        send(buf.at[s], s, z, yx)
        send(buf.at[s], s, z, cx)
    for zt in near:
        s = slot(zt, yx)
        arrived(s)
        send(buf.at[s], s, z, cx)
    for zt in (z, *near):
        arrived(slot(zt, cx))
        arrived(slot(zt, cyx))
    return started


def norm_scale(hb, count):
    def body(g, tot):
        h = hb[g].astype(F32)
        return tot + jnp.sum(h * h, axis=1, keepdims=True)

    tot = lax.fori_loop(0, count, body, jnp.zeros((hb.shape[1], 1), F32))
    return lax.rsqrt(tot / (count * hb.shape[2]) + NORM_EPS)


def normed(hb, gain_ref, g, r):
    w = hb.shape[2]
    gain = gain_ref[:, pl.ds(pl.multiple_of(g * w, w), w)].astype(F32)
    return (hb[g].astype(F32) * r * gain).astype(BF)


def qkv_kernel(h_ref, gain_ref, w_hbm, out_ref, hb, wbuf, acc, zloc, zbuf, wsem, ssem, rsem, ssem2, rsem2):
    z, x = lax.axis_index("yz"), lax.axis_index("x")
    me = z * 4 + x
    parts = [
        pltpu.make_async_copy(w_hbm.at[0, pl.ds(pl.multiple_of(x * 256, 256), 256), :], wbuf.at[pl.ds(0, 256), :], wsem.at[0]),
        pltpu.make_async_copy(w_hbm.at[0, pl.ds(1024, 64), :], wbuf.at[pl.ds(256, 64), :], wsem.at[1]),
        pltpu.make_async_copy(w_hbm.at[0, pl.ds(1024, 64), :], wbuf.at[pl.ds(320, 64), :], wsem.at[2]),
    ]
    for cp in parts:
        cp.start()
    group_barrier(z, x)
    hb[x * 4 + z] = h_ref[...]
    sent = gather(hb, lambda zt, xt: xt * 4 + zt, lambda zt: h_ref, ssem, rsem, z, x)
    r = norm_scale(hb, 16)
    acc[...] = jnp.zeros_like(acc)
    for cp in parts:
        cp.wait()

    def body(g, c):
        u = normed(hb, gain_ref, g, r)
        w = wbuf[:, pl.ds(pl.multiple_of(g * 256, 256), 256)]
        acc[...] += lax.dot_general(u, w, (((1,), (1,)), ((), ())), preferred_element_type=F32)
        return c

    lax.fori_loop(0, 16, body, 0)
    for d in range(16):
        zloc[d] = acc[d * 8:(d + 1) * 8, :].astype(BF)

    def peer(p):
        d = lax.rem(me + p, 16)
        return remote(zloc.at[d], zbuf.at[me], ssem2.at[p], rsem2.at[me], lax.div(d, 4), lax.rem(d, 4))

    def start(p, c):
        peer(p).start()
        return c

    def finish(p, c):
        peer(p).wait_send()
        d = lax.rem(me + p, 16)
        remote(zbuf.at[d], zbuf.at[d], ssem2.at[0], rsem2.at[d], z, x).wait_recv()
        return c

    lax.fori_loop(1, 16, start, 0)
    zbuf[me] = zloc[me]
    for cp in sent:
        cp.wait_send()
    lax.fori_loop(1, 16, finish, 0)
    out_ref[...] = zbuf[...]


def attn_kernel(len_ref, z_ref, k_hbm, v_hbm, o_ref, ko_hbm, vo_hbm, kbuf, vbuf, zrow, orow, isem, osem):
    rows, positions, hd = kbuf.shape

    def load(b, which):
        if which == 0:
            return pltpu.make_async_copy(k_hbm.at[0, b], kbuf.at[b], isem.at[0, b])
        return pltpu.make_async_copy(v_hbm.at[0, b], vbuf.at[b], isem.at[1, b])

    def store(b, which):
        if which == 0:
            return pltpu.make_async_copy(kbuf.at[b], ko_hbm.at[0, b], osem.at[0, b])
        return pltpu.make_async_copy(vbuf.at[b], vo_hbm.at[0, b], osem.at[1, b])

    def start(b, c):
        load(b, 0).start()
        load(b, 1).start()
        return c

    lax.fori_loop(0, rows, start, 0)
    lane = lax.broadcasted_iota(jnp.int32, (rows, hd), 1)
    for pair in range(2):
        base = 17 * pair
        even, odd = 8 * pair, 8 * pair + 4
        mains_e = [z_ref[even + i // 2, :, (i % 2) * hd:(i % 2 + 1) * hd].astype(F32) for i in range(8)]
        mains_o = [pltpu.roll(z_ref[odd + i // 2, :, (i % 2) * hd:(i % 2 + 1) * hd].astype(F32), hd // 2, 1) for i in range(8)]
        tail_e = z_ref[even, :, 2 * hd:3 * hd].astype(F32)
        tail_o = z_ref[odd, :, 2 * hd:3 * hd].astype(F32)
        heads = mains_e + [jnp.where(lane < hd // 2, tail_e, mains_o[0])]
        for i in range(8):
            heads.append(jnp.where(lane < hd // 2, mains_o[i], mains_o[i + 1] if i < 7 else tail_o))
        for i, v in enumerate(heads):
            zrow[:, base + i, :] = v
    heads = zrow.shape[1] - 2
    scale = hd ** -0.5

    def put(buf, b, row, pos):
        lo = pl.multiple_of(lax.div(pos, 16) * 16, 16)
        tile = buf[b, pl.ds(lo, 16), :].astype(F32)
        hit = lax.broadcasted_iota(jnp.int32, (16, hd), 0) == pos - lo
        buf[b, pl.ds(lo, 16), :] = jnp.where(hit, row, tile).astype(BF)

    def body(b, c):
        pos = len_ref[b]
        load(b, 0).wait()
        put(kbuf, b, zrow[b, heads:heads + 1, :], pos)
        q = zrow[b, 0:heads, :].astype(BF)
        s = lax.dot_general(q, kbuf[b], (((1,), (1,)), ((), ())), preferred_element_type=F32) * scale
        ids = lax.broadcasted_iota(jnp.int32, s.shape, 1)
        s = jnp.where(ids <= pos, s, -1e30)
        e = jnp.exp(s - jnp.max(s, axis=1, keepdims=True))
        p = (e / jnp.sum(e, axis=1, keepdims=True)).astype(BF)
        load(b, 1).wait()
        put(vbuf, b, zrow[b, heads + 1:heads + 2, :], pos)
        orow[b] = jnp.dot(p, vbuf[b], preferred_element_type=F32)
        store(b, 0).start()
        store(b, 1).start()
        return c

    lax.fori_loop(0, rows, body, 0)
    for h in range(heads):
        o_ref[h // 8, h % 8] = orow[:, h, :].astype(BF)

    def finish(b, c):
        store(b, 0).wait()
        store(b, 1).wait()
        return c

    lax.fori_loop(0, rows, finish, 0)


def mlp_kernel(o_ref, h_ref, gain_ref, wo_hbm, wg_hbm, wd_hbm, out_ref,
               wo, wg, wd, spread, obuf, olhs, part, recv, hb, acc, mbuf, part2, recv2,
               wsem, ssem_o, rsem_o, ssem_p, rsem_p, ssem_h, rsem_h, ssem_m, rsem_m, ssem_q, rsem_q):
    z, x = lax.axis_index("yz"), lax.axis_index("x")
    cols = pl.ds(pl.multiple_of(x * 1024, 1024), 1024)
    tiles = wg.shape[0]
    depth = wg.shape[1]
    flat = wg_hbm.at[0].reshape(depth, wg_hbm.shape[3])
    loads = [pltpu.make_async_copy(wo_hbm.at[0, :, cols], wo, wsem.at[0])]
    for j in range(tiles):
        lanes = pl.ds(pl.multiple_of((x * tiles + j) * 128, 128), 128)
        loads.append(pltpu.make_async_copy(flat.at[:, lanes], wg.at[j], wsem.at[1 + j]))
    loads.append(pltpu.make_async_copy(wd_hbm.at[0, :, cols], wd, wsem.at[1 + tiles]))
    for cp in loads:
        cp.start()
    group_barrier(z, x)

    k_id = lax.broadcasted_iota(jnp.int32, (256, 512), 0)
    c_id = lax.broadcasted_iota(jnp.int32, (256, 512), 1)
    spread[0] = jnp.where(c_id == 2 * k_id, 1.0, 0.0).astype(BF)
    spread[1] = jnp.where(c_id == 2 * k_id + 1, 1.0, 0.0).astype(BF)

    obuf[z * 4 + x] = o_ref[z]
    sent = gather(obuf, lambda zt, xt: zt * 4 + xt, lambda zt: o_ref.at[zt], ssem_o, rsem_o, z, x)
    for h in range(8):
        olhs[:, h * 128:(h + 1) * 128] = obuf[:, h].reshape(128, 128)

    def reduce_scatter(product, part, recv, ssem, rsem):
        copies = []
        for i, zt in enumerate(by_distance(z)):
            part[zt] = product(zt).astype(BF)
            cp = remote(part.at[zt], recv.at[z], ssem.at[i], rsem.at[z], zt, x)
            cp.start()
            copies.append(cp)
        total = product(z)
        for zt in by_distance(z):
            remote(recv.at[zt], recv.at[zt], ssem.at[0], rsem.at[zt], z, x).wait_recv()
            total += recv[zt].astype(F32)
        return total, copies

    loads[0].wait()

    def out_block(zt):
        return jnp.dot(olhs[...], wo[:, pl.ds(pl.multiple_of(zt * 256, 256), 256)], preferred_element_type=F32)

    total, more = reduce_scatter(out_block, part, recv, ssem_p, rsem_p)
    sent += more
    own = x * 4 + z
    hb[own] = (h_ref[...].astype(F32) + total).astype(BF)
    sent += gather(hb, lambda zt, xt: xt * 4 + zt, lambda zt: hb.at[own], ssem_h, rsem_h, z, x)
    r = norm_scale(hb, 16)
    acc[...] = jnp.zeros_like(acc)
    for j in range(tiles):
        loads[1 + j].wait()

    def body(g, c):
        u = normed(hb, gain_ref, g, r)
        even = jnp.dot(u, spread[0], preferred_element_type=F32).astype(BF)
        odd = jnp.dot(u, spread[1], preferred_element_type=F32).astype(BF)
        lhs = jnp.concatenate([even, odd], axis=0)
        rows = pl.ds(pl.multiple_of(g * 512, 512), 512)
        for j in range(0, tiles, 2):
            width = min(2, tiles - j)
            w = jnp.concatenate([wg[j + i, rows, :] for i in range(width)], axis=1)
            acc[:, j * 128:(j + width) * 128] += jnp.dot(lhs, w, preferred_element_type=F32)
        return c

    lax.fori_loop(0, 16, body, 0)
    gate = acc[0:128, :].astype(BF).astype(F32)
    up = acc[128:256, :].astype(BF).astype(F32)
    mbuf[x] = (jax.nn.silu(gate) * up).astype(BF)

    yx = lax.rem(x + 2, 4)
    cx = x + 1 - 2 * lax.rem(x, 2)
    cyx = lax.rem(cx + 2, 4)
    mcopies = [remote(mbuf.at[x], mbuf.at[x], ssem_m.at[0], rsem_m.at[x], z, yx),
               remote(mbuf.at[x], mbuf.at[x], ssem_m.at[1], rsem_m.at[x], z, cx)]
    for cp in mcopies:
        cp.start()
    remote(mbuf.at[yx], mbuf.at[yx], ssem_m.at[0], rsem_m.at[yx], z, x).wait_recv()
    cp = remote(mbuf.at[yx], mbuf.at[yx], ssem_m.at[2], rsem_m.at[yx], z, cx)
    cp.start()
    sent += mcopies + [cp]
    for xt in (cx, cyx):
        remote(mbuf.at[xt], mbuf.at[xt], ssem_m.at[0], rsem_m.at[xt], z, x).wait_recv()
    loads[1 + tiles].wait()

    def down_block(zt):
        lanes = pl.ds(pl.multiple_of(zt * 256, 256), 256)
        width = mbuf.shape[2]
        return functools.reduce(lambda a, b: a + b, [
            jnp.dot(mbuf[i], wd[i * width:(i + 1) * width, lanes], preferred_element_type=F32) for i in range(4)])

    total, more = reduce_scatter(down_block, part2, recv2, ssem_q, rsem_q)
    sent += more
    out_ref[...] = (hb[own].astype(F32) + total).astype(BF)
    for cp in sent:
        cp.wait_send()


def solution(mesh):
    hidden_spec = P('replica', ('x', 'yz'))
    batch_axes = ('replica', 'yz', 'x')
    cache_spec = P(None, batch_axes, None, None)
    vmem = pl.BlockSpec(memory_space=pltpu.VMEM)
    smem = pl.BlockSpec(memory_space=pltpu.SMEM)
    anywhere = pl.BlockSpec(memory_space=pl.ANY)
    dma, sd = pltpu.SemaphoreType.DMA, jax.ShapeDtypeStruct

    def layer(hidden, seq_lens, attn_gain, mlp_gain, w_qkv, w_out, w_gate_up, w_down, k_cache, v_cache):
        w_qkv_t = jnp.swapaxes(w_qkv, 1, 2)
        z_rows = pl.pallas_call(
            qkv_kernel,
            out_shape=sd((16, 8, 384), BF),
            in_specs=[vmem, vmem, anywhere],
            out_specs=vmem,
            scratch_shapes=[pltpu.VMEM((16, 128, 256), BF), pltpu.VMEM((384, 4096), BF), pltpu.VMEM((128, 384), F32),
                            pltpu.VMEM((16, 8, 384), BF), pltpu.VMEM((16, 8, 384), BF),
                            dma((3,)), dma((15,)), dma((16,)), dma((16,)), dma((16,))],
            compiler_params=pltpu.CompilerParams(collective_id=0, has_side_effects=True, vmem_limit_bytes=16 * MIB),
            name="qkv",
        )(hidden, attn_gain, w_qkv_t)
        rows, positions, hd = k_cache.shape[1:]
        o, k_out, v_out = pl.pallas_call(
            attn_kernel,
            out_shape=(sd((4, 8, rows, hd), BF), sd(k_cache.shape, BF), sd(v_cache.shape, BF)),
            in_specs=[smem, vmem, anywhere, anywhere],
            out_specs=(vmem, anywhere, anywhere),
            scratch_shapes=[pltpu.VMEM((rows, positions, hd), BF), pltpu.VMEM((rows, positions, hd), BF),
                            pltpu.VMEM((rows, 34, hd), F32), pltpu.VMEM((rows, 32, hd), F32),
                            dma((2, rows)), dma((2, rows))],
            compiler_params=pltpu.CompilerParams(vmem_limit_bytes=32 * MIB),
            name="attend",
        )(seq_lens, z_rows, k_cache, v_cache)
        hidden = pl.pallas_call(
            mlp_kernel,
            out_shape=sd(hidden.shape, BF),
            in_specs=[vmem, vmem, vmem, anywhere, anywhere, anywhere],
            out_specs=vmem,
            scratch_shapes=[pltpu.VMEM((1024, 1024), BF), pltpu.VMEM((7, 8192, 128), BF), pltpu.VMEM((3584, 1024), BF),
                            pltpu.VMEM((2, 256, 512), BF), pltpu.VMEM((16, 8, 8, 128), BF), pltpu.VMEM((128, 1024), BF),
                            pltpu.VMEM((4, 128, 256), BF), pltpu.VMEM((4, 128, 256), BF), pltpu.VMEM((16, 128, 256), BF),
                            pltpu.VMEM((256, 896), F32), pltpu.VMEM((4, 128, 896), BF),
                            pltpu.VMEM((4, 128, 256), BF), pltpu.VMEM((4, 128, 256), BF),
                            dma((9,)), dma((15,)), dma((16,)), dma((3,)), dma((4,)), dma((15,)), dma((16,)),
                            dma((3,)), dma((4,)), dma((3,)), dma((4,))],
            compiler_params=pltpu.CompilerParams(collective_id=1, has_side_effects=True, vmem_limit_bytes=56 * MIB),
            name="mlp",
        )(o, hidden, mlp_gain, w_out, w_gate_up, w_down)
        return hidden, k_out, v_out

    return jax.shard_map(
        layer,
        mesh=mesh,
        in_specs=(hidden_spec, P(batch_axes), P(), P(), P(None, None, 'yz'), P(None, 'yz', None),
                  P(None, None, None, 'yz'), P(None, 'yz', None), cache_spec, cache_spec),
        out_specs=(hidden_spec, cache_spec, cache_spec),
        check_vma=False)
```

```python
import functools

import jax
import jax.numpy as jnp
from jax import lax
from jax.experimental import pallas as pl
from jax.experimental.pallas import tpu as pltpu
from jax.sharding import PartitionSpec as P

NORM_EPS = 1e-5
MESH = pl.DeviceIdType.MESH
BF = jnp.bfloat16
F32 = jnp.float32
MIB = 1024 * 1024
UNROLL = 2


def at(z, x):
    return {"yz": z, "x": x}


def remote(src, dst, ssem, rsem, z, x):
    return pltpu.make_async_remote_copy(src_ref=src, dst_ref=dst, send_sem=ssem, recv_sem=rsem,
                                        device_id=at(z, x), device_id_type=MESH)


def group_barrier(z, x):
    sem = pltpu.get_barrier_semaphore()
    me = z * 4 + x

    def body(p, c):
        d = lax.rem(me + p, 16)
        pl.semaphore_signal(sem, inc=1, device_id=at(lax.div(d, 4), lax.rem(d, 4)), device_id_type=MESH)
        return c

    lax.fori_loop(1, 16, body, 0)
    pl.semaphore_wait(sem, 15)


def by_distance(z):
    a, b = lax.div(z, 2), lax.rem(z, 2)
    first = lax.div(z + 3, 4)
    n1 = first * (z - 1) + (1 - first)
    n2 = 2 + a * (1 - 2 * b)
    return n1, n2, 6 - z - n1 - n2


def gather(buf, slot, src_for, ssem, rsem, z, x, ready=None, consume=None):
    yx = lax.rem(x + 2, 4)
    cx = x + 1 - 2 * lax.rem(x, 2)
    cyx = lax.rem(cx + 2, 4)
    n1, n2, n3 = near = by_distance(z)
    me = slot(z, x)
    started = []

    def send(src, s, zt, xt):
        cp = remote(src, buf.at[s], ssem.at[len(started)], rsem.at[s], zt, xt)
        cp.start()
        started.append(cp)

    def arrived(s):
        remote(buf.at[s], buf.at[s], ssem.at[0], rsem.at[s], z, x).wait_recv()

    def pass_on(zt, xt, *targets):
        s = slot(zt, xt)
        arrived(s)
        for t in targets:
            send(buf.at[s], s, z, t)

    def work(first, second, *late):
        for zt, xt in late:
            arrived(slot(zt, xt))
        if consume is not None:
            s0, s1 = slot(*first), slot(*second)
            lax.fori_loop(0, 2, lambda i, c: (consume(s0 + i * (s1 - s0)), c)[1], 0)

    send(src_for(z), me, z, yx)
    for zt in near:
        send(src_for(zt), me, zt, x)
    send(src_for(z), me, z, cx)
    pass_on(z, yx, cx)
    pass_on(n1, x, yx, cx)
    if ready is not None:
        ready()
    work((z, x), (z, yx))
    pass_on(n2, x, yx, cx)
    work((n1, x), (z, cx), (z, cx))
    pass_on(n3, x, yx, cx)
    work((n2, x), (z, cyx), (z, cyx))
    pass_on(n1, yx, cx)
    work((n3, x), (n1, cx), (n1, cx))
    pass_on(n2, yx, cx)
    work((n1, yx), (n2, cx), (n2, cx))
    work((n2, yx), (n3, cx), (n3, cx))
    pass_on(n3, yx, cx)
    work((n3, yx), (n1, cyx), (n1, cyx))
    work((n2, cyx), (n3, cyx), (n2, cyx), (n3, cyx))
    return started


def share_sums(h, stat, ssem, rsem, z, x):
    me = z * 4 + x
    rows = h.shape[0]
    hf = h.astype(F32)
    sums = jnp.broadcast_to(jnp.sum(hf * hf, axis=1, keepdims=True), (rows, 128))
    stat[me] = jnp.transpose(sums)[0:1, :]

    def peer(p):
        d = lax.rem(me + p, 16)
        return remote(stat.at[me], stat.at[me], ssem.at[p], rsem.at[me], lax.div(d, 4), lax.rem(d, 4))

    def start(p, c):
        peer(p).start()
        return c

    lax.fori_loop(1, 16, start, 0)
    return peer


def scale_of(stat, peer, ssem, rsem, z, x, width):
    me = z * 4 + x

    def finish(p, c):
        peer(p).wait_send()
        d = lax.rem(me + p, 16)
        remote(stat.at[d], stat.at[d], ssem.at[0], rsem.at[d], z, x).wait_recv()
        return c

    lax.fori_loop(1, 16, finish, 0)
    tot = functools.reduce(lambda u, v: u + v, [stat[i] for i in range(16)])
    r = lax.rsqrt(tot / width + NORM_EPS)
    return jnp.transpose(jnp.broadcast_to(r, (128, 128)))[:, 0:1]


def normed(hb, gain_ref, g, r):
    w = hb.shape[2]
    gain = gain_ref[:, pl.ds(pl.multiple_of(g * w, w), w)].astype(F32)
    return (hb[g].astype(F32) * r * gain).astype(BF)


def qkv_kernel(h_ref, gain_ref, w_hbm, out_ref, hb, wbuf, acc, scale, stat, zloc, zbuf,
               wsem, ssem, rsem, ssem_s, rsem_s, ssem2, rsem2):
    z, x = lax.axis_index("yz"), lax.axis_index("x")
    me = z * 4 + x
    parts = [
        pltpu.make_async_copy(w_hbm.at[0, pl.ds(pl.multiple_of(x * 256, 256), 256), :], wbuf.at[pl.ds(0, 256), :], wsem.at[0]),
        pltpu.make_async_copy(w_hbm.at[0, pl.ds(1024, 64), :], wbuf.at[pl.ds(256, 64), :], wsem.at[1]),
        pltpu.make_async_copy(w_hbm.at[0, pl.ds(1024, 64), :], wbuf.at[pl.ds(320, 64), :], wsem.at[2]),
    ]
    for cp in parts:
        cp.start()
    hb[x * 4 + z] = h_ref[...]
    acc[...] = jnp.zeros_like(acc)
    group_barrier(z, x)
    peer_s = share_sums(h_ref[...], stat, ssem_s, rsem_s, z, x)

    def ready():
        scale[...] = scale_of(stat, peer_s, ssem_s, rsem_s, z, x, 4096)
        for cp in parts:
            cp.wait()

    def consume(g):
        u = normed(hb, gain_ref, g, scale[...])
        w = wbuf[:, pl.ds(pl.multiple_of(g * 256, 256), 256)]
        acc[...] += lax.dot_general(u, w, (((1,), (1,)), ((), ())), preferred_element_type=F32)

    sent = gather(hb, lambda zt, xt: xt * 4 + zt, lambda zt: h_ref, ssem, rsem, z, x, ready, consume)
    for d in range(16):
        zloc[d] = acc[d * 8:(d + 1) * 8, :].astype(BF)

    def peer(p):
        d = lax.rem(me + p, 16)
        return remote(zloc.at[d], zbuf.at[me], ssem2.at[p], rsem2.at[me], lax.div(d, 4), lax.rem(d, 4))

    def start(p, c):
        peer(p).start()
        return c

    def finish(p, c):
        peer(p).wait_send()
        d = lax.rem(me + p, 16)
        remote(zbuf.at[d], zbuf.at[d], ssem2.at[0], rsem2.at[d], z, x).wait_recv()
        return c

    lax.fori_loop(1, 16, start, 0)
    zbuf[me] = zloc[me]
    for cp in sent:
        cp.wait_send()
    lax.fori_loop(1, 16, finish, 0)
    out_ref[...] = zbuf[...]


def attn_kernel(len_ref, z_ref, k_ref, v_ref, o_ref, ko_hbm, vo_hbm, zrow, orow, tiles, osem, tsem):
    rows, positions, hd = k_ref.shape[1:]

    def store(b, which):
        src, dst = ((k_ref, ko_hbm), (v_ref, vo_hbm))[which]
        return pltpu.make_async_copy(src.at[0, b], dst.at[0, b], osem.at[which, b])

    def first(b):
        return pl.multiple_of(lax.div(len_ref[b], 16) * 16, 16)

    def patch(b, which):
        dst = (ko_hbm, vo_hbm)[which]
        return pltpu.make_async_copy(tiles.at[which, b], dst.at[0, b, pl.ds(first(b), 16), :], tsem.at[which, b])

    def start(b, c):
        store(b, 0).start()
        store(b, 1).start()
        return c

    lax.fori_loop(0, rows, start, 0)
    lane = lax.broadcasted_iota(jnp.int32, (rows, hd), 1)
    for pair in range(2):
        base = 17 * pair
        even, odd = 8 * pair, 8 * pair + 4
        mains_e = [z_ref[even + i // 2, :, (i % 2) * hd:(i % 2 + 1) * hd].astype(F32) for i in range(8)]
        mains_o = [pltpu.roll(z_ref[odd + i // 2, :, (i % 2) * hd:(i % 2 + 1) * hd].astype(F32), hd // 2, 1) for i in range(8)]
        tail_e = z_ref[even, :, 2 * hd:3 * hd].astype(F32)
        tail_o = z_ref[odd, :, 2 * hd:3 * hd].astype(F32)
        heads = mains_e + [jnp.where(lane < hd // 2, tail_e, mains_o[0])]
        for i in range(8):
            heads.append(jnp.where(lane < hd // 2, mains_o[i], mains_o[i + 1] if i < 7 else tail_o))
        for i, v in enumerate(heads):
            zrow[:, base + i, :] = v
    heads = zrow.shape[1] - 2
    factor = hd ** -0.5 * 1.4426950408889634

    def updated(ref, b, row, pos):
        lo = first(b)
        tile = ref[0, b, pl.ds(lo, 16), :].astype(F32)
        hit = lax.broadcasted_iota(jnp.int32, (16, hd), 0) == pos - lo
        return jnp.where(hit, row, tile).astype(BF)

    def one(b):
        pos = len_ref[b]
        k_new, v_new = zrow[b, heads:heads + 1, :], zrow[b, heads + 1:heads + 2, :]
        tiles[0, b] = updated(k_ref, b, k_new, pos)
        tiles[1, b] = updated(v_ref, b, v_new, pos)
        q = zrow[b, 0:heads, :]
        s = lax.dot_general(q.astype(BF), k_ref[0, b], (((1,), (1,)), ((), ())), preferred_element_type=F32)
        s_new = jnp.sum(q * k_new, axis=1, keepdims=True)
        ids = lax.broadcasted_iota(jnp.int32, s.shape, 1)
        s = jnp.where(ids < pos, s, -1e30)
        top = jnp.maximum(jnp.max(s, axis=1, keepdims=True), s_new)
        e = jnp.exp2((s - top) * factor)
        e_new = jnp.exp2((s_new - top) * factor)
        inv = 1.0 / (jnp.sum(e, axis=1, keepdims=True) + e_new)
        p = (e * inv).astype(BF)
        p_new = (e_new * inv).astype(BF).astype(F32)
        orow[b] = jnp.dot(p, v_ref[0, b], preferred_element_type=F32) + p_new * v_new

    def body(i, c):
        for k in range(UNROLL):
            one(i * UNROLL + k)
        return c

    lax.fori_loop(0, rows // UNROLL, body, 0)
    for h in range(heads):
        o_ref[h // 8, h % 8] = orow[:, h, :].astype(BF)

    def fix(b, c):
        for which in range(2):
            store(b, which).wait()
            patch(b, which).start()
        return c

    def finish(b, c):
        for which in range(2):
            patch(b, which).wait()
        return c

    lax.fori_loop(0, rows, fix, 0)
    lax.fori_loop(0, rows, finish, 0)


def mlp_kernel(o_ref, h_ref, gain_ref, wo_hbm, wg_hbm, wd_hbm, out_ref,
               wo, wg, wd, spread, obuf, olhs, part, recv, hb, acc, scale, stat, mbuf, part2, recv2,
               wsem, ssem_s, rsem_s, ssem_o, rsem_o, ssem_p, rsem_p, ssem_h, rsem_h, ssem_m, rsem_m, ssem_q, rsem_q):
    z, x = lax.axis_index("yz"), lax.axis_index("x")
    cols = pl.ds(pl.multiple_of(x * 1024, 1024), 1024)
    tiles = wg.shape[0]
    depth = wg.shape[1]
    flat = wg_hbm.at[0].reshape(depth, wg_hbm.shape[3])
    loads = [pltpu.make_async_copy(wo_hbm.at[0, :, cols], wo, wsem.at[0])]
    for j in range(tiles):
        lanes = pl.ds(pl.multiple_of((x * tiles + j) * 128, 128), 128)
        loads.append(pltpu.make_async_copy(flat.at[:, lanes], wg.at[j], wsem.at[1 + j]))
    loads.append(pltpu.make_async_copy(wd_hbm.at[0, :, cols], wd, wsem.at[1 + tiles]))
    for cp in loads:
        cp.start()
    group_barrier(z, x)

    k_id = lax.broadcasted_iota(jnp.int32, (256, 512), 0)
    c_id = lax.broadcasted_iota(jnp.int32, (256, 512), 1)
    spread[0] = jnp.where(c_id == 2 * k_id, 1.0, 0.0).astype(BF)
    spread[1] = jnp.where(c_id == 2 * k_id + 1, 1.0, 0.0).astype(BF)

    obuf[z * 4 + x] = o_ref[z]
    sent = gather(obuf, lambda zt, xt: zt * 4 + xt, lambda zt: o_ref.at[zt], ssem_o, rsem_o, z, x)
    for h in range(8):
        olhs[:, h * 128:(h + 1) * 128] = obuf[:, h].reshape(128, 128)

    def reduce_scatter(product, part, recv, ssem, rsem):
        copies = []
        for i, zt in enumerate(by_distance(z)):
            part[zt] = product(zt).astype(BF)
            cp = remote(part.at[zt], recv.at[z], ssem.at[i], rsem.at[z], zt, x)
            cp.start()
            copies.append(cp)
        total = product(z)
        for zt in by_distance(z):
            remote(recv.at[zt], recv.at[zt], ssem.at[0], rsem.at[zt], z, x).wait_recv()
            total += recv[zt].astype(F32)
        return total, copies

    loads[0].wait()

    def out_block(zt):
        return jnp.dot(olhs[...], wo[:, pl.ds(pl.multiple_of(zt * 256, 256), 256)], preferred_element_type=F32)

    total, more = reduce_scatter(out_block, part, recv, ssem_p, rsem_p)
    sent += more
    own = x * 4 + z
    hb[own] = (h_ref[...].astype(F32) + total).astype(BF)
    peer_s = share_sums(hb[own], stat, ssem_s, rsem_s, z, x)
    acc[...] = jnp.zeros_like(acc)

    def ready():
        scale[...] = scale_of(stat, peer_s, ssem_s, rsem_s, z, x, 4096)
        for j in range(tiles):
            loads[1 + j].wait()

    def consume(g):
        u = normed(hb, gain_ref, g, scale[...])
        even = jnp.dot(u, spread[0], preferred_element_type=F32).astype(BF)
        odd = jnp.dot(u, spread[1], preferred_element_type=F32).astype(BF)
        lhs = jnp.concatenate([even, odd], axis=0)
        rows = pl.ds(pl.multiple_of(g * 512, 512), 512)
        for j in range(0, tiles, 2):
            width = min(2, tiles - j)
            w = jnp.concatenate([wg[j + i, rows, :] for i in range(width)], axis=1)
            acc[:, j * 128:(j + width) * 128] += jnp.dot(lhs, w, preferred_element_type=F32)

    sent += gather(hb, lambda zt, xt: xt * 4 + zt, lambda zt: hb.at[own], ssem_h, rsem_h, z, x, ready, consume)
    gate = acc[0:128, :].astype(BF).astype(F32)
    up = acc[128:256, :].astype(BF).astype(F32)
    mbuf[x] = (jax.nn.silu(gate) * up).astype(BF)

    yx = lax.rem(x + 2, 4)
    cx = x + 1 - 2 * lax.rem(x, 2)
    cyx = lax.rem(cx + 2, 4)
    mcopies = [remote(mbuf.at[x], mbuf.at[x], ssem_m.at[0], rsem_m.at[x], z, yx),
               remote(mbuf.at[x], mbuf.at[x], ssem_m.at[1], rsem_m.at[x], z, cx)]
    for cp in mcopies:
        cp.start()
    remote(mbuf.at[yx], mbuf.at[yx], ssem_m.at[0], rsem_m.at[yx], z, x).wait_recv()
    cp = remote(mbuf.at[yx], mbuf.at[yx], ssem_m.at[2], rsem_m.at[yx], z, cx)
    cp.start()
    sent += mcopies + [cp]
    for xt in (cx, cyx):
        remote(mbuf.at[xt], mbuf.at[xt], ssem_m.at[0], rsem_m.at[xt], z, x).wait_recv()
    loads[1 + tiles].wait()

    def down_block(zt):
        lanes = pl.ds(pl.multiple_of(zt * 256, 256), 256)
        width = mbuf.shape[2]
        return functools.reduce(lambda a, b: a + b, [
            jnp.dot(mbuf[i], wd[i * width:(i + 1) * width, lanes], preferred_element_type=F32) for i in range(4)])

    total, more = reduce_scatter(down_block, part2, recv2, ssem_q, rsem_q)
    sent += more
    out_ref[...] = (hb[own].astype(F32) + total).astype(BF)
    for cp in sent:
        cp.wait_send()


def solution(mesh):
    hidden_spec = P('replica', ('x', 'yz'))
    batch_axes = ('replica', 'yz', 'x')
    cache_spec = P(None, batch_axes, None, None)
    vmem = pl.BlockSpec(memory_space=pltpu.VMEM)
    smem = pl.BlockSpec(memory_space=pltpu.SMEM)
    hbm = pl.BlockSpec(memory_space=pltpu.HBM)
    dma, sd = pltpu.SemaphoreType.DMA, jax.ShapeDtypeStruct

    def layer(hidden, seq_lens, attn_gain, mlp_gain, w_qkv, w_out, w_gate_up, w_down, k_cache, v_cache):
        w_qkv_t = jnp.swapaxes(w_qkv, 1, 2)
        z_rows = pl.pallas_call(
            qkv_kernel,
            out_shape=sd((16, 8, 384), BF),
            in_specs=[vmem, vmem, hbm],
            out_specs=vmem,
            scratch_shapes=[pltpu.VMEM((16, 128, 256), BF), pltpu.VMEM((384, 4096), BF), pltpu.VMEM((128, 384), F32),
                            pltpu.VMEM((128, 1), F32), pltpu.VMEM((16, 1, 128), F32),
                            pltpu.VMEM((16, 8, 384), BF), pltpu.VMEM((16, 8, 384), BF),
                            dma((3,)), dma((15,)), dma((16,)), dma((16,)), dma((16,)), dma((16,)), dma((16,))],
            compiler_params=pltpu.CompilerParams(collective_id=0, has_side_effects=True, vmem_limit_bytes=46 * MIB),
            cost_estimate=pl.CostEstimate(flops=30_000_000_000, bytes_accessed=20_000_000, transcendentals=0),
            name="qkv",
        )(hidden, attn_gain, w_qkv_t)
        rows, positions, hd = k_cache.shape[1:]
        o, k_out, v_out = pl.pallas_call(
            attn_kernel,
            out_shape=(sd((4, 8, rows, hd), BF), sd(k_cache.shape, BF), sd(v_cache.shape, BF)),
            in_specs=[smem, vmem, vmem, vmem],
            out_specs=(vmem, hbm, hbm),
            scratch_shapes=[pltpu.VMEM((rows, 34, hd), F32), pltpu.VMEM((rows, 32, hd), F32),
                            pltpu.VMEM((2, rows, 16, hd), BF), dma((2, rows)), dma((2, rows))],
            compiler_params=pltpu.CompilerParams(vmem_limit_bytes=28 * MIB),
            name="attend",
        )(seq_lens, z_rows, k_cache, v_cache)
        hidden = pl.pallas_call(
            mlp_kernel,
            out_shape=sd(hidden.shape, BF),
            in_specs=[vmem, vmem, vmem, hbm, hbm, hbm],
            out_specs=vmem,
            scratch_shapes=[pltpu.VMEM((1024, 1024), BF), pltpu.VMEM((7, 8192, 128), BF), pltpu.VMEM((3584, 1024), BF),
                            pltpu.VMEM((2, 256, 512), BF), pltpu.VMEM((16, 8, 8, 128), BF), pltpu.VMEM((128, 1024), BF),
                            pltpu.VMEM((4, 128, 256), BF), pltpu.VMEM((4, 128, 256), BF), pltpu.VMEM((16, 128, 256), BF),
                            pltpu.VMEM((256, 896), F32), pltpu.VMEM((128, 1), F32), pltpu.VMEM((16, 1, 128), F32),
                            pltpu.VMEM((4, 128, 896), BF),
                            pltpu.VMEM((4, 128, 256), BF), pltpu.VMEM((4, 128, 256), BF),
                            dma((9,)), dma((16,)), dma((16,)), dma((15,)), dma((16,)), dma((3,)), dma((4,)), dma((15,)), dma((16,)),
                            dma((3,)), dma((4,)), dma((3,)), dma((4,))],
            compiler_params=pltpu.CompilerParams(collective_id=1, has_side_effects=True, vmem_limit_bytes=56 * MIB),
            name="mlp",
        )(o, hidden, mlp_gain, w_out, w_gate_up, w_down)
        return hidden, k_out, v_out

    return jax.shard_map(
        layer,
        mesh=mesh,
        in_specs=(hidden_spec, P(batch_axes), P(), P(), P(None, None, 'yz'), P(None, 'yz', None),
                  P(None, None, None, 'yz'), P(None, 'yz', None), cache_spec, cache_spec),
        out_specs=(hidden_spec, cache_spec, cache_spec),
        check_vma=False)
```

```python
import functools

import jax
import jax.numpy as jnp
from jax import lax
from jax.experimental import pallas as pl
from jax.experimental.pallas import tpu as pltpu
from jax.sharding import PartitionSpec as P

NORM_EPS = 1e-5
MESH = pl.DeviceIdType.MESH
BF = jnp.bfloat16
F32 = jnp.float32
MIB = 1024 * 1024
UNROLL = 4


def at(z, x):
    return {"yz": z, "x": x}


def remote(src, dst, ssem, rsem, z, x):
    return pltpu.make_async_remote_copy(src_ref=src, dst_ref=dst, send_sem=ssem, recv_sem=rsem,
                                        device_id=at(z, x), device_id_type=MESH)


def group_barrier(z, x, between=None):
    sem = pltpu.get_barrier_semaphore()
    me = z * 4 + x

    def body(p, c):
        d = lax.rem(me + p, 16)
        pl.semaphore_signal(sem, inc=1, device_id=at(lax.div(d, 4), lax.rem(d, 4)), device_id_type=MESH)
        return c

    lax.fori_loop(1, 16, body, 0)
    if between is not None:
        between()
    pl.semaphore_wait(sem, 15)


def by_distance(z):
    a, b = lax.div(z, 2), lax.rem(z, 2)
    first = lax.div(z + 3, 4)
    n1 = first * (z - 1) + (1 - first)
    n2 = 2 + a * (1 - 2 * b)
    return n1, n2, 6 - z - n1 - n2


def gather(buf, slot, src_for, ssem, rsem, z, x, ready=None, consume=None):
    yx = lax.rem(x + 2, 4)
    cx = x + 1 - 2 * lax.rem(x, 2)
    cyx = lax.rem(cx + 2, 4)
    n1, n2, n3 = near = by_distance(z)
    me = slot(z, x)
    started = []

    def send(src, s, zt, xt):
        cp = remote(src, buf.at[s], ssem.at[len(started)], rsem.at[s], zt, xt)
        cp.start()
        started.append(cp)

    def arrived(s):
        remote(buf.at[s], buf.at[s], ssem.at[0], rsem.at[s], z, x).wait_recv()

    def pass_on(zt, xt, *targets):
        s = slot(zt, xt)
        arrived(s)
        for t in targets:
            send(buf.at[s], s, z, t)

    def work(first, second, *late):
        for zt, xt in late:
            arrived(slot(zt, xt))
        if consume is not None:
            consume(slot(*first), slot(*second))

    send(src_for(z), me, z, yx)
    for zt in near:
        send(src_for(zt), me, zt, x)
    send(src_for(z), me, z, cx)
    pass_on(z, yx, cx)
    pass_on(n1, x, yx, cx)
    if ready is not None:
        ready()
    work((z, x), (z, yx))
    pass_on(n2, x, yx, cx)
    work((n1, x), (z, cx), (z, cx))
    pass_on(n3, x, yx, cx)
    work((n2, x), (z, cyx), (z, cyx))
    pass_on(n1, yx, cx)
    work((n3, x), (n1, cx), (n1, cx))
    pass_on(n2, yx, cx)
    work((n1, yx), (n2, cx), (n2, cx))
    work((n2, yx), (n3, cx), (n3, cx))
    pass_on(n3, yx, cx)
    work((n3, yx), (n1, cyx), (n1, cyx))
    work((n2, cyx), (n3, cyx), (n2, cyx), (n3, cyx))
    return started


def share_sums(h, stat, ssem, rsem, z, x):
    me = z * 4 + x
    rows = h.shape[0]
    hf = h.astype(F32)
    sums = jnp.broadcast_to(jnp.sum(hf * hf, axis=1, keepdims=True), (rows, 128))
    stat[me] = jnp.transpose(sums)[0:1, :]

    def peer(p):
        d = lax.rem(me + p, 16)
        return remote(stat.at[me], stat.at[me], ssem.at[p], rsem.at[me], lax.div(d, 4), lax.rem(d, 4))

    def start(p, c):
        peer(p).start()
        return c

    lax.fori_loop(1, 16, start, 0)
    return peer


def scale_of(stat, peer, ssem, rsem, z, x, width):
    me = z * 4 + x

    def finish(p, c):
        peer(p).wait_send()
        d = lax.rem(me + p, 16)
        remote(stat.at[d], stat.at[d], ssem.at[0], rsem.at[d], z, x).wait_recv()
        return c

    lax.fori_loop(1, 16, finish, 0)
    tot = functools.reduce(lambda u, v: u + v, [stat[i] for i in range(16)])
    r = lax.rsqrt(tot / width + NORM_EPS)
    return jnp.transpose(jnp.broadcast_to(r, (128, 128)))[:, 0:1]


def normed(hb, gain, g, r):
    w = hb.shape[2]
    return (hb[g].astype(F32) * r * gain[:, pl.ds(pl.multiple_of(g * w, w), w)].astype(F32)).astype(BF)


def qkv_kernel(h_hbm, gain_hbm, w_hbm, out_ref, h_ref, gain, hb, wbuf, acc, scale, stat, zloc, zbuf,
               wsem, ssem, rsem, ssem_s, rsem_s, ssem2, rsem2):
    z, x = lax.axis_index("yz"), lax.axis_index("x")
    me = z * 4 + x
    parts = [
        pltpu.make_async_copy(w_hbm.at[0, pl.ds(pl.multiple_of(x * 256, 256), 256), :], wbuf.at[pl.ds(0, 256), :], wsem.at[0]),
        pltpu.make_async_copy(w_hbm.at[0, pl.ds(1024, 64), :], wbuf.at[pl.ds(256, 64), :], wsem.at[1]),
        pltpu.make_async_copy(w_hbm.at[0, pl.ds(1024, 64), :], wbuf.at[pl.ds(320, 64), :], wsem.at[2]),
        pltpu.make_async_copy(gain_hbm, gain, wsem.at[3]),
    ]
    mine = pltpu.make_async_copy(h_hbm, h_ref, wsem.at[4])
    mine.start()
    for cp in parts:
        cp.start()
    acc[...] = jnp.zeros_like(acc)
    group_barrier(z, x, mine.wait)
    hb[x * 4 + z] = h_ref[...]
    peer_s = share_sums(h_ref[...], stat, ssem_s, rsem_s, z, x)

    def ready():
        scale[...] = scale_of(stat, peer_s, ssem_s, rsem_s, z, x, 4096)
        for cp in parts:
            cp.wait()

    def consume(*pair):
        u = jnp.concatenate([normed(hb, gain, g, scale[...]) for g in pair], axis=1)
        w = jnp.concatenate([wbuf[:, pl.ds(pl.multiple_of(g * 256, 256), 256)] for g in pair], axis=1)
        acc[...] += lax.dot_general(u, w, (((1,), (1,)), ((), ())), preferred_element_type=F32)

    sent = gather(hb, lambda zt, xt: xt * 4 + zt, lambda zt: h_ref, ssem, rsem, z, x, ready, consume)
    for d in range(16):
        zloc[d] = acc[d * 8:(d + 1) * 8, :].astype(BF)

    def peer(p):
        d = lax.rem(me + p, 16)
        return remote(zloc.at[d], zbuf.at[me], ssem2.at[p], rsem2.at[me], lax.div(d, 4), lax.rem(d, 4))

    def start(p, c):
        peer(p).start()
        return c

    def finish(p, c):
        peer(p).wait_send()
        d = lax.rem(me + p, 16)
        remote(zbuf.at[d], zbuf.at[d], ssem2.at[0], rsem2.at[d], z, x).wait_recv()
        return c

    lax.fori_loop(1, 16, start, 0)
    zbuf[me] = zloc[me]
    for cp in sent:
        cp.wait_send()
    lax.fori_loop(1, 16, finish, 0)
    out_ref[...] = zbuf[...]


def attn_kernel(len_ref, z_ref, k_ref, v_ref, o_ref, ko_hbm, vo_hbm, zrow, orow, tiles, osem, tsem):
    rows, positions, hd = k_ref.shape[1:]

    def store(b, which):
        src, dst = ((k_ref, ko_hbm), (v_ref, vo_hbm))[which]
        return pltpu.make_async_copy(src.at[0, b], dst.at[0, b], osem.at[which, b])

    def first(b):
        return pl.multiple_of(lax.div(len_ref[b], 16) * 16, 16)

    def patch(b, which):
        dst = (ko_hbm, vo_hbm)[which]
        return pltpu.make_async_copy(tiles.at[which, b], dst.at[0, b, pl.ds(first(b), 16), :], tsem.at[which, b])

    def start(b, c):
        store(b, 0).start()
        store(b, 1).start()
        return c

    lax.fori_loop(0, rows, start, 0)
    lane = lax.broadcasted_iota(jnp.int32, (rows, hd), 1)
    for pair in range(2):
        base = 17 * pair
        even, odd = 8 * pair, 8 * pair + 4
        mains_e = [z_ref[even + i // 2, :, (i % 2) * hd:(i % 2 + 1) * hd].astype(F32) for i in range(8)]
        mains_o = [pltpu.roll(z_ref[odd + i // 2, :, (i % 2) * hd:(i % 2 + 1) * hd].astype(F32), hd // 2, 1) for i in range(8)]
        tail_e = z_ref[even, :, 2 * hd:3 * hd].astype(F32)
        tail_o = z_ref[odd, :, 2 * hd:3 * hd].astype(F32)
        heads = mains_e + [jnp.where(lane < hd // 2, tail_e, mains_o[0])]
        for i in range(8):
            heads.append(jnp.where(lane < hd // 2, mains_o[i], mains_o[i + 1] if i < 7 else tail_o))
        for i, v in enumerate(heads):
            zrow[:, base + i, :] = v
    heads = zrow.shape[1] - 2
    factor = hd ** -0.5 * 1.4426950408889634

    def updated(ref, b, row, pos):
        lo = first(b)
        tile = ref[0, b, pl.ds(lo, 16), :].astype(F32)
        hit = lax.broadcasted_iota(jnp.int32, (16, hd), 0) == pos - lo
        return jnp.where(hit, row, tile).astype(BF)

    def one(b):
        pos = len_ref[b]
        k_new, v_new = zrow[b, heads:heads + 1, :], zrow[b, heads + 1:heads + 2, :]
        tiles[0, b] = updated(k_ref, b, k_new, pos)
        tiles[1, b] = updated(v_ref, b, v_new, pos)
        q = zrow[b, 0:heads, :]
        s = lax.dot_general(q.astype(BF), k_ref[0, b], (((1,), (1,)), ((), ())), preferred_element_type=F32)
        s_new = jnp.sum(q * k_new, axis=1, keepdims=True)
        ids = lax.broadcasted_iota(jnp.int32, s.shape, 1)
        s = jnp.where(ids < pos, s, -1e30)
        top = jnp.maximum(jnp.max(s, axis=1, keepdims=True), s_new)
        e = jnp.exp2((s - top) * factor)
        e_new = jnp.exp2((s_new - top) * factor)
        inv = 1.0 / (jnp.sum(e, axis=1, keepdims=True) + e_new)
        p = (e * inv).astype(BF)
        p_new = (e_new * inv).astype(BF).astype(F32)
        orow[b] = jnp.dot(p, v_ref[0, b], preferred_element_type=F32) + p_new * v_new

    def fix(b):
        for which in range(2):
            store(b, which).wait()
            patch(b, which).start()

    def body(i, c):
        for k in range(UNROLL):
            one(i * UNROLL + k)
        for k in range(UNROLL):
            fix(i * UNROLL + k)
        return c

    lax.fori_loop(0, rows // UNROLL, body, 0)
    for h in range(heads):
        o_ref[h // 8, h % 8] = orow[:, h, :].astype(BF)

    def finish(b, c):
        for which in range(2):
            patch(b, which).wait()
        return c

    lax.fori_loop(0, rows, finish, 0)


def mlp_kernel(o_hbm, h_hbm, gain_hbm, wo_hbm, wg_hbm, wd_hbm, out_ref,
               o_ref, h_ref, gain, wo, wg, wd, spread, obuf, olhs, part, recv, hb, acc, scale, stat, mbuf, part2, recv2, total2,
               wsem, ssem_s, rsem_s, ssem_o, rsem_o, ssem_p, rsem_p, ssem_h, rsem_h, ssem_m, rsem_m, ssem_q, rsem_q):
    z, x = lax.axis_index("yz"), lax.axis_index("x")
    cols = pl.ds(pl.multiple_of(x * 1024, 1024), 1024)
    tiles = wg.shape[0]
    depth = wg.shape[1]
    flat = wg_hbm.at[0].reshape(depth, wg_hbm.shape[3])
    small = [pltpu.make_async_copy(o_hbm, o_ref, wsem.at[2 + tiles]), pltpu.make_async_copy(h_hbm, h_ref, wsem.at[3 + tiles]),
             pltpu.make_async_copy(gain_hbm, gain, wsem.at[4 + tiles])]
    for cp in small:
        cp.start()
    loads = [pltpu.make_async_copy(wo_hbm.at[0, :, cols], wo, wsem.at[0])]
    for j in range(tiles):
        lanes = pl.ds(pl.multiple_of((x * tiles + j) * 128, 128), 128)
        loads.append(pltpu.make_async_copy(flat.at[:, lanes], wg.at[j], wsem.at[1 + j]))
    loads.append(pltpu.make_async_copy(wd_hbm.at[0, :, cols], wd, wsem.at[1 + tiles]))
    for cp in loads:
        cp.start()
    k_id = lax.broadcasted_iota(jnp.int32, (256, 512), 0)
    c_id = lax.broadcasted_iota(jnp.int32, (256, 512), 1)
    spread[0] = jnp.where(c_id == 2 * k_id, 1.0, 0.0).astype(BF)
    spread[1] = jnp.where(c_id == 2 * k_id + 1, 1.0, 0.0).astype(BF)
    acc[...] = jnp.zeros_like(acc)

    def settle():
        for cp in small:
            cp.wait()

    group_barrier(z, x, settle)
    yx = lax.rem(x + 2, 4)
    cx = x + 1 - 2 * lax.rem(x, 2)
    cyx = lax.rem(cx + 2, 4)
    near = by_distance(z)

    sent = []
    mine = z * 4 + x
    places = [(z, yx)] + [(zt, xt) for zt in near for xt in (x, yx)]

    def o_send(src, s, zt, xt):
        cp = remote(src, obuf.at[s], ssem_o.at[len(sent)], rsem_o.at[s], zt, xt)
        cp.start()
        sent.append(cp)

    def o_arrived(zt, xt):
        s = zt * 4 + xt
        remote(obuf.at[s], obuf.at[s], ssem_o.at[0], rsem_o.at[s], z, x).wait_recv()

    for zt, xt in places:
        o_send(o_ref.at[zt], mine, zt, xt)
    o_send(o_ref.at[z], mine, z, cx)
    obuf[mine] = o_ref[z]
    for zt, xt in places:
        o_arrived(zt, xt)
        o_send(obuf.at[zt * 4 + xt], zt * 4 + xt, z, cx)
    for zt in (z, *near):
        o_arrived(zt, cx)
        o_arrived(zt, cyx)
    for h in range(8):
        olhs[:, h * 128:(h + 1) * 128] = obuf[:, h].reshape(128, 128)

    loads[0].wait()

    def out_block(zt):
        return jnp.dot(olhs[...], wo[:, pl.ds(pl.multiple_of(zt * 256, 256), 256)], preferred_element_type=F32)

    for i, zt in enumerate(near):
        part[zt] = out_block(zt).astype(BF)
        cp = remote(part.at[zt], recv.at[z], ssem_p.at[i], rsem_p.at[z], zt, x)
        cp.start()
        sent.append(cp)
    total = out_block(z)
    for zt in near:
        remote(recv.at[zt], recv.at[zt], ssem_p.at[0], rsem_p.at[zt], z, x).wait_recv()
        total += recv[zt].astype(F32)
    own = x * 4 + z
    hb[own] = (h_ref[...].astype(F32) + total).astype(BF)
    peer_s = share_sums(hb[own], stat, ssem_s, rsem_s, z, x)

    def ready():
        scale[...] = scale_of(stat, peer_s, ssem_s, rsem_s, z, x, 4096)
        for j in range(tiles):
            loads[1 + j].wait()

    def consume(*pair):
        lhs = []
        for g in pair:
            u = normed(hb, gain, g, scale[...])
            even = jnp.dot(u, spread[0], preferred_element_type=F32).astype(BF)
            odd = jnp.dot(u, spread[1], preferred_element_type=F32).astype(BF)
            lhs.append(jnp.concatenate([even, odd], axis=0))
        lhs = jnp.concatenate(lhs, axis=1)
        for j in range(0, tiles, 2):
            width = min(2, tiles - j)
            w = jnp.concatenate([
                jnp.concatenate([wg[j + i, pl.ds(pl.multiple_of(g * 512, 512), 512), :] for i in range(width)], axis=1)
                for g in pair], axis=0)
            acc[:, j * 128:(j + width) * 128] += jnp.dot(lhs, w, preferred_element_type=F32)

    sent += gather(hb, lambda zt, xt: xt * 4 + zt, lambda zt: hb.at[own], ssem_h, rsem_h, z, x, ready, consume)
    gate = acc[0:128, :].astype(BF).astype(F32)
    up = acc[128:256, :].astype(BF).astype(F32)
    m = (jax.nn.silu(gate) * up).astype(BF)
    halves, half = mbuf.shape[0], mbuf.shape[2]
    for f in range(halves):
        mbuf[f, x] = m[f * half:(f + 1) * half, :]

    def m_send(f, xt, target, i):
        cp = remote(mbuf.at[f, xt], mbuf.at[f, xt], ssem_m.at[f, i], rsem_m.at[f, xt], z, target)
        cp.start()
        sent.append(cp)

    def m_arrived(f, xt):
        remote(mbuf.at[f, xt], mbuf.at[f, xt], ssem_m.at[f, 0], rsem_m.at[f, xt], z, x).wait_recv()

    for f in range(halves):
        m_send(f, x, yx, 0)
        m_send(f, x, cx, 1)
    loads[1 + tiles].wait()

    def down_block(f, zt):
        lanes = pl.ds(pl.multiple_of(zt * 256, 256), 256)
        width = mbuf.shape[3]
        return functools.reduce(lambda a, b: a + b, [
            jnp.dot(mbuf[f, i], wd[i * width:(i + 1) * width, lanes], preferred_element_type=F32) for i in range(4)])

    for f in range(halves):
        m_arrived(f, yx)
        m_send(f, yx, cx, 2)
        m_arrived(f, cx)
        m_arrived(f, cyx)
        for i, zt in enumerate(near):
            part2[f, zt] = down_block(f, zt).astype(BF)
            cp = remote(part2.at[f, zt], recv2.at[f, z], ssem_q.at[f, i], rsem_q.at[f, z], zt, x)
            cp.start()
            sent.append(cp)
        total2[f] = down_block(f, z)
    for f in range(halves):
        total = total2[f]
        for zt in near:
            remote(recv2.at[f, zt], recv2.at[f, zt], ssem_q.at[f, 0], rsem_q.at[f, zt], z, x).wait_recv()
            total += recv2[f, zt].astype(F32)
        rows = slice(f * half, (f + 1) * half)
        out_ref[rows, :] = (hb[own, rows, :].astype(F32) + total).astype(BF)
    for cp in sent:
        cp.wait_send()


def solution(mesh):
    hidden_spec = P('replica', ('x', 'yz'))
    batch_axes = ('replica', 'yz', 'x')
    cache_spec = P(None, batch_axes, None, None)
    vmem = pl.BlockSpec(memory_space=pltpu.VMEM)
    smem = pl.BlockSpec(memory_space=pltpu.SMEM)
    hbm = pl.BlockSpec(memory_space=pltpu.HBM)
    dma, sd = pltpu.SemaphoreType.DMA, jax.ShapeDtypeStruct

    def layer(hidden, seq_lens, attn_gain, mlp_gain, w_qkv, w_out, w_gate_up, w_down, k_cache, v_cache):
        w_qkv_t = jnp.swapaxes(w_qkv, 1, 2)
        z_rows = pl.pallas_call(
            qkv_kernel,
            out_shape=sd((16, 8, 384), BF),
            in_specs=[hbm, hbm, hbm],
            out_specs=vmem,
            scratch_shapes=[pltpu.VMEM((128, 256), BF), pltpu.VMEM((1, 4096), BF), pltpu.VMEM((16, 128, 256), BF), pltpu.VMEM((384, 4096), BF), pltpu.VMEM((128, 384), F32),
                            pltpu.VMEM((128, 1), F32), pltpu.VMEM((16, 1, 128), F32),
                            pltpu.VMEM((16, 8, 384), BF), pltpu.VMEM((16, 8, 384), BF),
                            dma((5,)), dma((15,)), dma((16,)), dma((16,)), dma((16,)), dma((16,)), dma((16,))],
            compiler_params=pltpu.CompilerParams(collective_id=0, has_side_effects=True, vmem_limit_bytes=46 * MIB),
            cost_estimate=pl.CostEstimate(flops=30_000_000_000, bytes_accessed=20_000_000, transcendentals=0),
            name="qkv",
        )(hidden, attn_gain, w_qkv_t)
        rows, positions, hd = k_cache.shape[1:]
        o, k_out, v_out = pl.pallas_call(
            attn_kernel,
            out_shape=(sd((4, 8, rows, hd), BF), sd(k_cache.shape, BF), sd(v_cache.shape, BF)),
            in_specs=[smem, vmem, vmem, vmem],
            out_specs=(vmem, hbm, hbm),
            scratch_shapes=[pltpu.VMEM((rows, 34, hd), F32), pltpu.VMEM((rows, 32, hd), F32),
                            pltpu.VMEM((2, rows, 16, hd), BF), dma((2, rows)), dma((2, rows))],
            compiler_params=pltpu.CompilerParams(vmem_limit_bytes=28 * MIB),
            name="attend",
        )(seq_lens, z_rows, k_cache, v_cache)
        hidden = pl.pallas_call(
            mlp_kernel,
            out_shape=sd(hidden.shape, BF),
            in_specs=[hbm] * 6,
            out_specs=vmem,
            scratch_shapes=[pltpu.VMEM((4, 8, 8, 128), BF), pltpu.VMEM((128, 256), BF), pltpu.VMEM((1, 4096), BF),
                            pltpu.VMEM((1024, 1024), BF), pltpu.VMEM((7, 8192, 128), BF), pltpu.VMEM((3584, 1024), BF),
                            pltpu.VMEM((2, 256, 512), BF), pltpu.VMEM((16, 8, 8, 128), BF), pltpu.VMEM((128, 1024), BF),
                            pltpu.VMEM((4, 128, 256), BF), pltpu.VMEM((4, 128, 256), BF), pltpu.VMEM((16, 128, 256), BF),
                            pltpu.VMEM((256, 896), F32), pltpu.VMEM((128, 1), F32), pltpu.VMEM((16, 1, 128), F32),
                            pltpu.VMEM((2, 4, 64, 896), BF),
                            pltpu.VMEM((2, 4, 64, 256), BF), pltpu.VMEM((2, 4, 64, 256), BF), pltpu.VMEM((2, 64, 256), F32),
                            dma((12,)), dma((16,)), dma((16,)), dma((15,)), dma((16,)), dma((3,)), dma((4,)), dma((15,)), dma((16,)),
                            dma((2, 3)), dma((2, 4)), dma((2, 3)), dma((2, 4))],
            compiler_params=pltpu.CompilerParams(collective_id=1, has_side_effects=True, vmem_limit_bytes=56 * MIB),
            name="mlp",
        )(o, hidden, mlp_gain, w_out, w_gate_up, w_down)
        return hidden, k_out, v_out

    return jax.shard_map(
        layer,
        mesh=mesh,
        in_specs=(hidden_spec, P(batch_axes), P(), P(), P(None, None, 'yz'), P(None, 'yz', None),
                  P(None, None, None, 'yz'), P(None, 'yz', None), cache_spec, cache_spec),
        out_specs=(hidden_spec, cache_spec, cache_spec),
        check_vma=False)
```

```python
import functools

import jax
import jax.numpy as jnp
from jax import lax
from jax.experimental import pallas as pl
from jax.experimental.pallas import tpu as pltpu
from jax.sharding import PartitionSpec as P

NORM_EPS = 1e-5
MESH = pl.DeviceIdType.MESH
BF = jnp.bfloat16
F32 = jnp.float32
MIB = 1024 * 1024
UNROLL = 2


def at(z, x):
    return {"yz": z, "x": x}


def remote(src, dst, ssem, rsem, z, x):
    return pltpu.make_async_remote_copy(src_ref=src, dst_ref=dst, send_sem=ssem, recv_sem=rsem,
                                        device_id=at(z, x), device_id_type=MESH)


def group_barrier(z, x, between=None):
    sem = pltpu.get_barrier_semaphore()
    me = z * 4 + x

    def body(p, c):
        d = lax.rem(me + p, 16)
        pl.semaphore_signal(sem, inc=1, device_id=at(lax.div(d, 4), lax.rem(d, 4)), device_id_type=MESH)
        return c

    lax.fori_loop(1, 16, body, 0)
    if between is not None:
        between()
    pl.semaphore_wait(sem, 15)


def by_distance(z):
    a, b = lax.div(z, 2), lax.rem(z, 2)
    first = lax.div(z + 3, 4)
    n1 = first * (z - 1) + (1 - first)
    n2 = 2 + a * (1 - 2 * b)
    return n1, n2, 6 - z - n1 - n2


def gather(buf, slot, src_for, ssem, rsem, z, x, sent_own, ready, consume):
    yx = lax.rem(x + 2, 4)
    cx = x + 1 - 2 * lax.rem(x, 2)
    cyx = lax.rem(cx + 2, 4)
    n1, n2, n3 = near = by_distance(z)
    me = slot(z, x)
    started = []

    def send(src, s, zt, xt):
        cp = remote(src, buf.at[s], ssem.at[len(started)], rsem.at[s], zt, xt)
        cp.start()
        started.append(cp)

    def arrived(s):
        remote(buf.at[s], buf.at[s], ssem.at[0], rsem.at[s], z, x).wait_recv()

    def pass_on(zt, xt, *targets):
        s = slot(zt, xt)
        arrived(s)
        for t in targets:
            send(buf.at[s], s, z, t)

    def work(first, second, *late):
        for zt, xt in late:
            arrived(slot(zt, xt))
        consume(slot(*first), slot(*second))

    for zt in reversed(near):
        send(src_for(zt), me, zt, x)
    send(src_for(z), me, z, yx)
    send(src_for(z), me, z, cx)
    sent_own()
    pass_on(z, yx, cx)
    pass_on(n1, x, yx, cx)
    ready()
    work((z, x), (z, yx))
    pass_on(n2, x, yx, cx)
    work((n1, x), (z, cx), (z, cx))
    pass_on(n3, x, yx, cx)
    work((n2, x), (z, cyx), (z, cyx))
    pass_on(n1, yx, cx)
    work((n3, x), (n1, cx), (n1, cx))
    pass_on(n2, yx, cx)
    work((n1, yx), (n2, cx), (n2, cx))
    work((n2, yx), (n3, cx), (n3, cx))
    pass_on(n3, yx, cx)
    work((n3, yx), (n1, cyx), (n1, cyx))
    work((n2, cyx), (n3, cyx), (n2, cyx), (n3, cyx))
    return started


def share_sums(h, stat, ssem, rsem, z, x):
    me = z * 4 + x
    rows = h.shape[0]
    hf = h.astype(F32)
    sums = jnp.broadcast_to(jnp.sum(hf * hf, axis=1, keepdims=True), (rows, 128))
    stat[me] = jnp.transpose(sums)[0:1, :]

    def peer(p):
        d = lax.rem(me + p, 16)
        return remote(stat.at[me], stat.at[me], ssem.at[p], rsem.at[me], lax.div(d, 4), lax.rem(d, 4))

    def start(p, c):
        peer(p).start()
        return c

    lax.fori_loop(1, 16, start, 0)


def scale_of(stat, ssem, rsem, z, x, width):
    me = z * 4 + x

    def finish(p, c):
        remote(stat.at[me], stat.at[me], ssem.at[p], rsem.at[me], z, x).wait_send()
        d = lax.rem(me + p, 16)
        remote(stat.at[d], stat.at[d], ssem.at[0], rsem.at[d], z, x).wait_recv()
        return c

    lax.fori_loop(1, 16, finish, 0)
    tot = functools.reduce(lambda u, v: u + v, [stat[i] for i in range(16)])
    r = lax.rsqrt(tot / width + NORM_EPS)
    return jnp.transpose(jnp.broadcast_to(r, (128, 128)))[:, 0:1]


def normed(hb, gain, g, r):
    w = hb.shape[2]
    return (hb[g].astype(F32) * r * gain[:, pl.ds(pl.multiple_of(g * w, w), w)].astype(F32)).astype(BF)


def qkv_kernel(h_hbm, gain_hbm, w_hbm, out_ref, h_ref, gain, hb, wbuf, acc, scale, stat, zloc, zbuf,
               wsem, ssem, rsem, ssem_s, rsem_s, ssem2, rsem2):
    z, x = lax.axis_index("yz"), lax.axis_index("x")
    me = z * 4 + x
    parts = [
        pltpu.make_async_copy(w_hbm.at[0, pl.ds(pl.multiple_of(x * 256, 256), 256), :], wbuf.at[pl.ds(0, 256), :], wsem.at[0]),
        pltpu.make_async_copy(w_hbm.at[0, pl.ds(1024, 64), :], wbuf.at[pl.ds(256, 64), :], wsem.at[1]),
        pltpu.make_async_copy(w_hbm.at[0, pl.ds(1024, 64), :], wbuf.at[pl.ds(320, 64), :], wsem.at[2]),
        pltpu.make_async_copy(gain_hbm, gain, wsem.at[3]),
    ]
    mine = pltpu.make_async_copy(h_hbm, h_ref, wsem.at[4])
    mine.start()
    for cp in parts:
        cp.start()
    acc[...] = jnp.zeros_like(acc)
    group_barrier(z, x, mine.wait)

    def sent_own():
        share_sums(h_ref[...], stat, ssem_s, rsem_s, z, x)
        hb[x * 4 + z] = h_ref[...]

    def ready():
        scale[...] = scale_of(stat, ssem_s, rsem_s, z, x, 4096)
        for cp in parts:
            cp.wait()

    def consume(*pair):
        u = jnp.concatenate([normed(hb, gain, g, scale[...]) for g in pair], axis=1)
        w = jnp.concatenate([wbuf[:, pl.ds(pl.multiple_of(g * 256, 256), 256)] for g in pair], axis=1)
        acc[...] += lax.dot_general(u, w, (((1,), (1,)), ((), ())), preferred_element_type=F32)

    sent = gather(hb, lambda zt, xt: xt * 4 + zt, lambda zt: h_ref, ssem, rsem, z, x, sent_own, ready, consume)
    for d in range(16):
        zloc[d] = acc[d * 8:(d + 1) * 8, :].astype(BF)

    def peer(p):
        d = lax.rem(me + p, 16)
        return remote(zloc.at[d], zbuf.at[me], ssem2.at[p], rsem2.at[me], lax.div(d, 4), lax.rem(d, 4))

    def start(p, c):
        peer(p).start()
        return c

    def finish(p, c):
        peer(p).wait_send()
        d = lax.rem(me + p, 16)
        remote(zbuf.at[d], zbuf.at[d], ssem2.at[0], rsem2.at[d], z, x).wait_recv()
        return c

    lax.fori_loop(1, 16, start, 0)
    zbuf[me] = zloc[me]
    for cp in sent:
        cp.wait_send()
    lax.fori_loop(1, 16, finish, 0)
    out_ref[...] = zbuf[...]


def attn_kernel(len_ref, z_ref, k_ref, v_ref, o_ref, ko_hbm, vo_hbm, zrow, orow, tiles, osem, tsem):
    rows, positions, hd = k_ref.shape[1:]

    def store(b, which):
        src, dst = ((k_ref, ko_hbm), (v_ref, vo_hbm))[which]
        return pltpu.make_async_copy(src.at[0, b], dst.at[0, b], osem.at[which, b])

    def first(b):
        return pl.multiple_of(lax.div(len_ref[b], 16) * 16, 16)

    def patch(b, which):
        dst = (ko_hbm, vo_hbm)[which]
        return pltpu.make_async_copy(tiles.at[which, b], dst.at[0, b, pl.ds(first(b), 16), :], tsem.at[which, b])

    def start(b, c):
        store(b, 0).start()
        store(b, 1).start()
        return c

    lax.fori_loop(0, rows, start, 0)
    lane = lax.broadcasted_iota(jnp.int32, (rows, hd), 1)
    for pair in range(2):
        base = 17 * pair
        even, odd = 8 * pair, 8 * pair + 4
        mains_e = [z_ref[even + i // 2, :, (i % 2) * hd:(i % 2 + 1) * hd].astype(F32) for i in range(8)]
        mains_o = [pltpu.roll(z_ref[odd + i // 2, :, (i % 2) * hd:(i % 2 + 1) * hd].astype(F32), hd // 2, 1) for i in range(8)]
        tail_e = z_ref[even, :, 2 * hd:3 * hd].astype(F32)
        tail_o = z_ref[odd, :, 2 * hd:3 * hd].astype(F32)
        heads = mains_e + [jnp.where(lane < hd // 2, tail_e, mains_o[0])]
        for i in range(8):
            heads.append(jnp.where(lane < hd // 2, mains_o[i], mains_o[i + 1] if i < 7 else tail_o))
        for i, v in enumerate(heads):
            zrow[:, base + i, :] = v
    heads = zrow.shape[1] - 2
    factor = hd ** -0.5 * 1.4426950408889634

    def updated(ref, b, row, pos):
        lo = first(b)
        tile = ref[0, b, pl.ds(lo, 16), :].astype(F32)
        hit = lax.broadcasted_iota(jnp.int32, (16, hd), 0) == pos - lo
        return jnp.where(hit, row, tile).astype(BF)

    def renew(b, c):
        tiles[0, b] = updated(k_ref, b, zrow[b, heads:heads + 1, :], len_ref[b])
        tiles[1, b] = updated(v_ref, b, zrow[b, heads + 1:heads + 2, :], len_ref[b])
        return c

    lax.fori_loop(0, rows, renew, 0)

    def one(b):
        pos = len_ref[b]
        k_new, v_new = zrow[b, heads:heads + 1, :], zrow[b, heads + 1:heads + 2, :]
        q = zrow[b, 0:heads, :]
        s = lax.dot_general(q.astype(BF), k_ref[0, b], (((1,), (1,)), ((), ())), preferred_element_type=F32)
        s_new = jnp.sum(q * k_new, axis=1, keepdims=True)
        ids = lax.broadcasted_iota(jnp.int32, s.shape, 1)
        s = jnp.where(ids < pos, s, -1e30)
        top = jnp.maximum(jnp.max(s, axis=1, keepdims=True), s_new)
        e = jnp.exp2((s - top) * factor)
        e_new = jnp.exp2((s_new - top) * factor)
        inv = 1.0 / (jnp.sum(e, axis=1, keepdims=True) + e_new)
        p = (e * inv).astype(BF)
        p_new = (e_new * inv).astype(BF).astype(F32)
        orow[b] = jnp.dot(p, v_ref[0, b], preferred_element_type=F32) + p_new * v_new

    def fix(b):
        for which in range(2):
            store(b, which).wait()
            patch(b, which).start()

    def body(i, c):
        for k in range(UNROLL):
            one(i * UNROLL + k)
        return c

    def patches(b, c):
        fix(b)
        return c

    lax.fori_loop(0, rows // UNROLL - 1, body, 0)
    for b in range(rows - UNROLL, rows - 1):
        one(b)
    lax.fori_loop(0, rows, patches, 0)
    one(rows - 1)
    for h in range(heads):
        o_ref[h // 8, h % 8] = orow[:, h, :].astype(BF)

    def finish(b, c):
        for which in range(2):
            patch(b, which).wait()
        return c

    lax.fori_loop(0, rows, finish, 0)


def mlp_kernel(o_hbm, h_hbm, gain_hbm, wo_hbm, wg_hbm, wd_hbm, out_ref,
               o_ref, h_ref, gain, wo, wg, wd, spread, obuf, olhs, part, recv, hb, acc, scale, stat, mbuf, part2, recv2, total2,
               wsem, ssem_s, rsem_s, ssem_o, rsem_o, ssem_p, rsem_p, ssem_h, rsem_h, ssem_m, rsem_m, ssem_q, rsem_q):
    z, x = lax.axis_index("yz"), lax.axis_index("x")
    cols = pl.ds(pl.multiple_of(x * 1024, 1024), 1024)
    tiles = wg.shape[0]
    depth = wg.shape[1]
    flat = wg_hbm.at[0].reshape(depth, wg_hbm.shape[3])
    small = [pltpu.make_async_copy(o_hbm, o_ref, wsem.at[2 + tiles]), pltpu.make_async_copy(h_hbm, h_ref, wsem.at[3 + tiles]),
             pltpu.make_async_copy(gain_hbm, gain, wsem.at[4 + tiles])]
    for cp in small:
        cp.start()
    loads = [pltpu.make_async_copy(wo_hbm.at[0, :, cols], wo, wsem.at[0])]
    for j in range(tiles):
        lanes = pl.ds(pl.multiple_of((x * tiles + j) * 128, 128), 128)
        loads.append(pltpu.make_async_copy(flat.at[:, lanes], wg.at[j], wsem.at[1 + j]))
    loads.append(pltpu.make_async_copy(wd_hbm.at[0, :, cols], wd, wsem.at[1 + tiles]))
    for cp in loads:
        cp.start()
    k_id = lax.broadcasted_iota(jnp.int32, (256, 512), 0)
    c_id = lax.broadcasted_iota(jnp.int32, (256, 512), 1)
    spread[0] = jnp.where(c_id == 2 * k_id, 1.0, 0.0).astype(BF)
    spread[1] = jnp.where(c_id == 2 * k_id + 1, 1.0, 0.0).astype(BF)
    acc[...] = jnp.zeros_like(acc)

    def settle():
        for cp in small:
            cp.wait()

    group_barrier(z, x, settle)
    yx = lax.rem(x + 2, 4)
    cx = x + 1 - 2 * lax.rem(x, 2)
    cyx = lax.rem(cx + 2, 4)
    near = by_distance(z)

    sent = []
    mine = z * 4 + x
    places = [(z, yx)] + [(zt, xt) for zt in near for xt in (x, yx)]

    def o_send(src, s, zt, xt):
        cp = remote(src, obuf.at[s], ssem_o.at[len(sent)], rsem_o.at[s], zt, xt)
        cp.start()
        sent.append(cp)

    def o_arrived(zt, xt):
        s = zt * 4 + xt
        remote(obuf.at[s], obuf.at[s], ssem_o.at[0], rsem_o.at[s], z, x).wait_recv()

    for zt, xt in reversed(places):
        o_send(o_ref.at[zt], mine, zt, xt)
    o_send(o_ref.at[z], mine, z, cx)
    obuf[mine] = o_ref[z]
    for zt, xt in places:
        o_arrived(zt, xt)
        o_send(obuf.at[zt * 4 + xt], zt * 4 + xt, z, cx)
    for zt in (z, *near):
        o_arrived(zt, cx)
        o_arrived(zt, cyx)
    for h in range(8):
        olhs[:, h * 128:(h + 1) * 128] = obuf[:, h].reshape(128, 128)

    loads[0].wait()

    def out_block(zt):
        return jnp.dot(olhs[...], wo[:, pl.ds(pl.multiple_of(zt * 256, 256), 256)], preferred_element_type=F32)

    for i, zt in enumerate(reversed(near)):
        part[zt] = out_block(zt).astype(BF)
        cp = remote(part.at[zt], recv.at[z], ssem_p.at[i], rsem_p.at[z], zt, x)
        cp.start()
        sent.append(cp)
    total = out_block(z)
    for zt in near:
        remote(recv.at[zt], recv.at[zt], ssem_p.at[0], rsem_p.at[zt], z, x).wait_recv()
        total += recv[zt].astype(F32)
    own = x * 4 + z
    hb[own] = (h_ref[...].astype(F32) + total).astype(BF)

    def sent_own():
        share_sums(hb[own], stat, ssem_s, rsem_s, z, x)

    def ready():
        scale[...] = scale_of(stat, ssem_s, rsem_s, z, x, 4096)
        for j in range(tiles):
            loads[1 + j].wait()

    def consume(*pair):
        lhs = []
        for g in pair:
            u = normed(hb, gain, g, scale[...])
            even = jnp.dot(u, spread[0], preferred_element_type=F32).astype(BF)
            odd = jnp.dot(u, spread[1], preferred_element_type=F32).astype(BF)
            lhs.append(jnp.concatenate([even, odd], axis=0))
        lhs = jnp.concatenate(lhs, axis=1)
        for j in range(0, tiles, 2):
            width = min(2, tiles - j)
            w = jnp.concatenate([
                jnp.concatenate([wg[j + i, pl.ds(pl.multiple_of(g * 512, 512), 512), :] for i in range(width)], axis=1)
                for g in pair], axis=0)
            acc[:, j * 128:(j + width) * 128] += jnp.dot(lhs, w, preferred_element_type=F32)

    sent += gather(hb, lambda zt, xt: xt * 4 + zt, lambda zt: hb.at[own], ssem_h, rsem_h, z, x, sent_own, ready, consume)
    halves, half = mbuf.shape[0], mbuf.shape[2]

    def m_send(f, xt, target, i):
        cp = remote(mbuf.at[f, xt], mbuf.at[f, xt], ssem_m.at[f, i], rsem_m.at[f, xt], z, target)
        cp.start()
        sent.append(cp)

    def m_arrived(f, xt):
        remote(mbuf.at[f, xt], mbuf.at[f, xt], ssem_m.at[f, 0], rsem_m.at[f, xt], z, x).wait_recv()

    for f in range(halves):
        gate = acc[f * half:(f + 1) * half, :].astype(BF).astype(F32)
        up = acc[128 + f * half:128 + (f + 1) * half, :].astype(BF).astype(F32)
        mbuf[f, x] = (jax.nn.silu(gate) * up).astype(BF)
        m_send(f, x, yx, 0)
        m_send(f, x, cx, 1)
    loads[1 + tiles].wait()

    def down_block(f, zt):
        lanes = pl.ds(pl.multiple_of(zt * 256, 256), 256)
        width = mbuf.shape[3]
        return functools.reduce(lambda a, b: a + b, [
            jnp.dot(mbuf[f, i], wd[i * width:(i + 1) * width, lanes], preferred_element_type=F32) for i in range(4)])

    for f in range(halves):
        m_arrived(f, yx)
        m_send(f, yx, cx, 2)
        m_arrived(f, cx)
        m_arrived(f, cyx)
        for i, zt in enumerate(reversed(near)):
            part2[f, zt] = down_block(f, zt).astype(BF)
            cp = remote(part2.at[f, zt], recv2.at[f, z], ssem_q.at[f, i], rsem_q.at[f, z], zt, x)
            cp.start()
            sent.append(cp)
        total2[f] = down_block(f, z)
    for f in range(halves):
        total = total2[f]
        for zt in near:
            remote(recv2.at[f, zt], recv2.at[f, zt], ssem_q.at[f, 0], rsem_q.at[f, zt], z, x).wait_recv()
            total += recv2[f, zt].astype(F32)
        rows = slice(f * half, (f + 1) * half)
        out_ref[rows, :] = (hb[own, rows, :].astype(F32) + total).astype(BF)
    for cp in sent:
        cp.wait_send()


def solution(mesh):
    hidden_spec = P('replica', ('x', 'yz'))
    batch_axes = ('replica', 'yz', 'x')
    cache_spec = P(None, batch_axes, None, None)
    vmem = pl.BlockSpec(memory_space=pltpu.VMEM)
    smem = pl.BlockSpec(memory_space=pltpu.SMEM)
    hbm = pl.BlockSpec(memory_space=pltpu.HBM)
    dma, sd = pltpu.SemaphoreType.DMA, jax.ShapeDtypeStruct

    def layer(hidden, seq_lens, attn_gain, mlp_gain, w_qkv, w_out, w_gate_up, w_down, k_cache, v_cache):
        w_qkv_t = jnp.swapaxes(w_qkv, 1, 2)
        z_rows = pl.pallas_call(
            qkv_kernel,
            out_shape=sd((16, 8, 384), BF),
            in_specs=[hbm, hbm, hbm],
            out_specs=vmem,
            scratch_shapes=[pltpu.VMEM((128, 256), BF), pltpu.VMEM((1, 4096), BF), pltpu.VMEM((16, 128, 256), BF), pltpu.VMEM((384, 4096), BF), pltpu.VMEM((128, 384), F32),
                            pltpu.VMEM((128, 1), F32), pltpu.VMEM((16, 1, 128), F32),
                            pltpu.VMEM((16, 8, 384), BF), pltpu.VMEM((16, 8, 384), BF),
                            dma((5,)), dma((15,)), dma((16,)), dma((16,)), dma((16,)), dma((16,)), dma((16,))],
            compiler_params=pltpu.CompilerParams(collective_id=0, has_side_effects=True, vmem_limit_bytes=46 * MIB),
            cost_estimate=pl.CostEstimate(flops=30_000_000_000, bytes_accessed=20_000_000, transcendentals=0),
            name="qkv",
        )(hidden, attn_gain, w_qkv_t)
        rows, positions, hd = k_cache.shape[1:]
        o, k_out, v_out = pl.pallas_call(
            attn_kernel,
            out_shape=(sd((4, 8, rows, hd), BF), sd(k_cache.shape, BF), sd(v_cache.shape, BF)),
            in_specs=[smem, vmem, vmem, vmem],
            out_specs=(vmem, hbm, hbm),
            scratch_shapes=[pltpu.VMEM((rows, 34, hd), F32), pltpu.VMEM((rows, 32, hd), F32),
                            pltpu.VMEM((2, rows, 16, hd), BF), dma((2, rows)), dma((2, rows))],
            compiler_params=pltpu.CompilerParams(vmem_limit_bytes=28 * MIB),
            name="attend",
        )(seq_lens, z_rows, k_cache, v_cache)
        hidden = pl.pallas_call(
            mlp_kernel,
            out_shape=sd(hidden.shape, BF),
            in_specs=[hbm] * 6,
            out_specs=vmem,
            scratch_shapes=[pltpu.VMEM((4, 8, 8, 128), BF), pltpu.VMEM((128, 256), BF), pltpu.VMEM((1, 4096), BF),
                            pltpu.VMEM((1024, 1024), BF), pltpu.VMEM((7, 8192, 128), BF), pltpu.VMEM((3584, 1024), BF),
                            pltpu.VMEM((2, 256, 512), BF), pltpu.VMEM((16, 8, 8, 128), BF), pltpu.VMEM((128, 1024), BF),
                            pltpu.VMEM((4, 128, 256), BF), pltpu.VMEM((4, 128, 256), BF), pltpu.VMEM((16, 128, 256), BF),
                            pltpu.VMEM((256, 896), F32), pltpu.VMEM((128, 1), F32), pltpu.VMEM((16, 1, 128), F32),
                            pltpu.VMEM((2, 4, 64, 896), BF),
                            pltpu.VMEM((2, 4, 64, 256), BF), pltpu.VMEM((2, 4, 64, 256), BF), pltpu.VMEM((2, 64, 256), F32),
                            dma((12,)), dma((16,)), dma((16,)), dma((15,)), dma((16,)), dma((3,)), dma((4,)), dma((15,)), dma((16,)),
                            dma((2, 3)), dma((2, 4)), dma((2, 3)), dma((2, 4))],
            compiler_params=pltpu.CompilerParams(collective_id=1, has_side_effects=True, vmem_limit_bytes=48 * MIB),
            name="mlp",
        )(o, hidden, mlp_gain, w_out, w_gate_up, w_down)
        return hidden, k_out, v_out

    return jax.shard_map(
        layer,
        mesh=mesh,
        in_specs=(hidden_spec, P(batch_axes), P(), P(), P(None, None, 'yz'), P(None, 'yz', None),
                  P(None, None, None, 'yz'), P(None, 'yz', None), cache_spec, cache_spec),
        out_specs=(hidden_spec, cache_spec, cache_spec),
        check_vma=False)
```

```python
import functools

import jax
import jax.numpy as jnp
from jax import lax
from jax.experimental import pallas as pl
from jax.experimental.pallas import tpu as pltpu
from jax.sharding import PartitionSpec as P

NORM_EPS = 1e-5
MESH = pl.DeviceIdType.MESH
BF = jnp.bfloat16
F32 = jnp.float32
MIB = 1024 * 1024
UNROLL = 2


def at(z, x):
    return {"yz": z, "x": x}


def remote(src, dst, ssem, rsem, z, x):
    return pltpu.make_async_remote_copy(src_ref=src, dst_ref=dst, send_sem=ssem, recv_sem=rsem,
                                        device_id=at(z, x), device_id_type=MESH)


def group_barrier(z, x, between=None):
    sem = pltpu.get_barrier_semaphore()
    me = z * 4 + x

    def body(p, c):
        d = lax.rem(me + p, 16)
        pl.semaphore_signal(sem, inc=1, device_id=at(lax.div(d, 4), lax.rem(d, 4)), device_id_type=MESH)
        return c

    lax.fori_loop(1, 16, body, 0)
    if between is not None:
        between()
    pl.semaphore_wait(sem, 15)


def by_distance(z):
    a, b = lax.div(z, 2), lax.rem(z, 2)
    first = lax.div(z + 3, 4)
    n1 = first * (z - 1) + (1 - first)
    n2 = 2 + a * (1 - 2 * b)
    return n1, n2, 6 - z - n1 - n2


def gather(buf, slot, src_for, ssem, rsem, z, x, ready, consume):
    yx = lax.rem(x + 2, 4)
    cx = x + 1 - 2 * lax.rem(x, 2)
    cyx = lax.rem(cx + 2, 4)
    n1, n2, n3 = near = by_distance(z)
    me = slot(z, x)
    started = []

    def send(src, s, zt, xt):
        cp = remote(src, buf.at[s], ssem.at[len(started)], rsem.at[s], zt, xt)
        cp.start()
        started.append(cp)

    def arrived(s):
        remote(buf.at[s], buf.at[s], ssem.at[0], rsem.at[s], z, x).wait_recv()

    def pass_on(zt, xt, *targets):
        s = slot(zt, xt)
        arrived(s)
        for t in targets:
            send(buf.at[s], s, z, t)

    def work(first, second, *late):
        for zt, xt in late:
            arrived(slot(zt, xt))
        consume(slot(*first), slot(*second))

    send(src_for(z), me, z, yx)
    for zt in near:
        send(src_for(zt), me, zt, x)
    send(src_for(z), me, z, cx)
    pass_on(z, yx, cx)
    pass_on(n1, x, yx, cx)
    ready()
    work((z, x), (z, yx))
    pass_on(n2, x, yx, cx)
    work((n1, x), (z, cx), (z, cx))
    pass_on(n3, x, yx, cx)
    work((n2, x), (z, cyx), (z, cyx))
    pass_on(n1, yx, cx)
    work((n3, x), (n1, cx), (n1, cx))
    pass_on(n2, yx, cx)
    work((n1, yx), (n2, cx), (n2, cx))
    work((n2, yx), (n3, cx), (n3, cx))
    pass_on(n3, yx, cx)
    work((n3, yx), (n1, cyx), (n1, cyx))
    work((n2, cyx), (n3, cyx), (n2, cyx), (n3, cyx))
    return started


def share_sums(h, stat, ssem, rsem, z, x):
    me = z * 4 + x
    rows = h.shape[0]
    hf = h.astype(F32)
    sums = jnp.broadcast_to(jnp.sum(hf * hf, axis=1, keepdims=True), (rows, 128))
    stat[me] = jnp.transpose(sums)[0:1, :]

    def peer(p):
        d = lax.rem(me + p, 16)
        return remote(stat.at[me], stat.at[me], ssem.at[p], rsem.at[me], lax.div(d, 4), lax.rem(d, 4))

    def start(p, c):
        peer(p).start()
        return c

    lax.fori_loop(1, 16, start, 0)


def scale_of(stat, ssem, rsem, z, x, width):
    me = z * 4 + x

    def finish(p, c):
        remote(stat.at[me], stat.at[me], ssem.at[p], rsem.at[me], z, x).wait_send()
        d = lax.rem(me + p, 16)
        remote(stat.at[d], stat.at[d], ssem.at[0], rsem.at[d], z, x).wait_recv()
        return c

    lax.fori_loop(1, 16, finish, 0)
    tot = functools.reduce(lambda u, v: u + v, [stat[i] for i in range(16)])
    r = lax.rsqrt(tot / width + NORM_EPS)
    return jnp.transpose(jnp.broadcast_to(r, (128, 128)))[:, 0:1]


def normed(hb, gain, g, r):
    w = hb.shape[2]
    return (hb[g].astype(F32) * r * gain[:, pl.ds(pl.multiple_of(g * w, w), w)].astype(F32)).astype(BF)


def qkv_kernel(h_hbm, gain_hbm, w_hbm, out_ref, h_ref, gain, hb, wbuf, acc, scale, stat, zloc, zbuf,
               wsem, ssem, rsem, ssem_s, rsem_s, ssem2, rsem2):
    z, x = lax.axis_index("yz"), lax.axis_index("x")
    me = z * 4 + x
    parts = [
        pltpu.make_async_copy(w_hbm.at[0, pl.ds(pl.multiple_of(x * 256, 256), 256), :], wbuf.at[pl.ds(0, 256), :], wsem.at[0]),
        pltpu.make_async_copy(w_hbm.at[0, pl.ds(1024, 64), :], wbuf.at[pl.ds(256, 64), :], wsem.at[1]),
        pltpu.make_async_copy(w_hbm.at[0, pl.ds(1024, 64), :], wbuf.at[pl.ds(320, 64), :], wsem.at[2]),
        pltpu.make_async_copy(gain_hbm, gain, wsem.at[3]),
    ]
    mine = pltpu.make_async_copy(h_hbm, h_ref, wsem.at[4])
    mine.start()
    for cp in parts:
        cp.start()
    acc[...] = jnp.zeros_like(acc)
    group_barrier(z, x, mine.wait)
    share_sums(h_ref[...], stat, ssem_s, rsem_s, z, x)
    hb[x * 4 + z] = h_ref[...]

    def ready():
        scale[...] = scale_of(stat, ssem_s, rsem_s, z, x, 4096)
        for cp in parts:
            cp.wait()

    def consume(*pair):
        u = jnp.concatenate([normed(hb, gain, g, scale[...]) for g in pair], axis=1)
        w = jnp.concatenate([wbuf[:, pl.ds(pl.multiple_of(g * 256, 256), 256)] for g in pair], axis=1)
        acc[...] += lax.dot_general(u, w, (((1,), (1,)), ((), ())), preferred_element_type=F32)

    sent = gather(hb, lambda zt, xt: xt * 4 + zt, lambda zt: h_ref, ssem, rsem, z, x, ready, consume)
    for d in range(16):
        zloc[d] = acc[d * 8:(d + 1) * 8, :].astype(BF)

    def peer(p):
        d = lax.rem(me + p, 16)
        return remote(zloc.at[d], zbuf.at[me], ssem2.at[p], rsem2.at[me], lax.div(d, 4), lax.rem(d, 4))

    def start(p, c):
        peer(p).start()
        return c

    def finish(p, c):
        peer(p).wait_send()
        d = lax.rem(me + p, 16)
        remote(zbuf.at[d], zbuf.at[d], ssem2.at[0], rsem2.at[d], z, x).wait_recv()
        return c

    lax.fori_loop(1, 16, start, 0)
    zbuf[me] = zloc[me]
    for cp in sent:
        cp.wait_send()
    lax.fori_loop(1, 16, finish, 0)
    out_ref[...] = zbuf[...]


def attn_kernel(len_ref, z_ref, k_ref, v_ref, o_ref, ko_hbm, vo_hbm, zrow, orow, tiles, osem, tsem):
    rows, positions, hd = k_ref.shape[1:]

    def store(b, which):
        src, dst = ((k_ref, ko_hbm), (v_ref, vo_hbm))[which]
        return pltpu.make_async_copy(src.at[0, b], dst.at[0, b], osem.at[which, b])

    def first(b):
        return pl.multiple_of(lax.div(len_ref[b], 16) * 16, 16)

    def patch(b, which):
        dst = (ko_hbm, vo_hbm)[which]
        return pltpu.make_async_copy(tiles.at[which, b], dst.at[0, b, pl.ds(first(b), 16), :], tsem.at[which, b])

    def start(b, c):
        store(b, 0).start()
        store(b, 1).start()
        return c

    lax.fori_loop(0, rows, start, 0)
    lane = lax.broadcasted_iota(jnp.int32, (rows, hd), 1)
    for pair in range(2):
        base = 17 * pair
        even, odd = 8 * pair, 8 * pair + 4
        mains_e = [z_ref[even + i // 2, :, (i % 2) * hd:(i % 2 + 1) * hd].astype(F32) for i in range(8)]
        mains_o = [pltpu.roll(z_ref[odd + i // 2, :, (i % 2) * hd:(i % 2 + 1) * hd].astype(F32), hd // 2, 1) for i in range(8)]
        tail_e = z_ref[even, :, 2 * hd:3 * hd].astype(F32)
        tail_o = z_ref[odd, :, 2 * hd:3 * hd].astype(F32)
        heads = mains_e + [jnp.where(lane < hd // 2, tail_e, mains_o[0])]
        for i in range(8):
            heads.append(jnp.where(lane < hd // 2, mains_o[i], mains_o[i + 1] if i < 7 else tail_o))
        for i, v in enumerate(heads):
            zrow[:, base + i, :] = v
    heads = zrow.shape[1] - 2
    factor = hd ** -0.5 * 1.4426950408889634

    def updated(ref, b, row, pos):
        lo = first(b)
        tile = ref[0, b, pl.ds(lo, 16), :].astype(F32)
        hit = lax.broadcasted_iota(jnp.int32, (16, hd), 0) == pos - lo
        return jnp.where(hit, row, tile).astype(BF)

    def renew(b, c):
        tiles[0, b] = updated(k_ref, b, zrow[b, heads:heads + 1, :], len_ref[b])
        tiles[1, b] = updated(v_ref, b, zrow[b, heads + 1:heads + 2, :], len_ref[b])
        return c

    lax.fori_loop(0, rows, renew, 0)

    def one(b):
        pos = len_ref[b]
        k_new, v_new = zrow[b, heads:heads + 1, :], zrow[b, heads + 1:heads + 2, :]
        q = zrow[b, 0:heads, :]
        s = lax.dot_general(q.astype(BF), k_ref[0, b], (((1,), (1,)), ((), ())), preferred_element_type=F32)
        s_new = jnp.sum(q * k_new, axis=1, keepdims=True)
        ids = lax.broadcasted_iota(jnp.int32, s.shape, 1)
        s = jnp.where(ids < pos, s, -1e30)
        top = jnp.maximum(jnp.max(s, axis=1, keepdims=True), s_new)
        e = jnp.exp2((s - top) * factor)
        e_new = jnp.exp2((s_new - top) * factor)
        inv = 1.0 / (jnp.sum(e, axis=1, keepdims=True) + e_new)
        p = (e * inv).astype(BF)
        p_new = (e_new * inv).astype(BF).astype(F32)
        orow[b] = jnp.dot(p, v_ref[0, b], preferred_element_type=F32) + p_new * v_new

    def fix(b):
        for which in range(2):
            store(b, which).wait()
            patch(b, which).start()

    def body(i, c):
        for k in range(UNROLL):
            one(i * UNROLL + k)
        return c

    def patches(b, c):
        fix(b)
        return c

    lax.fori_loop(0, rows // UNROLL - 1, body, 0)
    for b in range(rows - UNROLL, rows - 1):
        one(b)
    lax.fori_loop(0, rows, patches, 0)
    one(rows - 1)
    for h in range(heads):
        o_ref[h // 8, h % 8] = orow[:, h, :].astype(BF)

    def finish(b, c):
        for which in range(2):
            patch(b, which).wait()
        return c

    lax.fori_loop(0, rows, finish, 0)


def mlp_kernel(o_hbm, h_hbm, gain_hbm, wo_hbm, wg_hbm, wd_hbm, out_ref,
               o_ref, h_ref, gain, wo, wg, wd, spread, obuf, olhs, part, recv, hb, acc, scale, stat, mbuf, low, part2, recv2,
               wsem, ssem_s, rsem_s, ssem_o, rsem_o, ssem_p, rsem_p, ssem_h, rsem_h, ssem_m, rsem_m, ssem_q, rsem_q):
    z, x = lax.axis_index("yz"), lax.axis_index("x")
    cols = pl.ds(pl.multiple_of(x * 1024, 1024), 1024)
    tiles = wg.shape[0]
    depth = wg.shape[1]
    flat = wg_hbm.at[0].reshape(depth, wg_hbm.shape[3])
    small = [pltpu.make_async_copy(o_hbm, o_ref, wsem.at[2 + tiles]), pltpu.make_async_copy(h_hbm, h_ref, wsem.at[3 + tiles]),
             pltpu.make_async_copy(gain_hbm, gain, wsem.at[4 + tiles])]
    for cp in small:
        cp.start()
    loads = [pltpu.make_async_copy(wo_hbm.at[0, :, cols], wo, wsem.at[0])]
    for j in range(tiles):
        lanes = pl.ds(pl.multiple_of((x * tiles + j) * 128, 128), 128)
        loads.append(pltpu.make_async_copy(flat.at[:, lanes], wg.at[j], wsem.at[1 + j]))
    loads.append(pltpu.make_async_copy(wd_hbm.at[0, :, cols], wd, wsem.at[1 + tiles]))
    for cp in loads:
        cp.start()
    k_id = lax.broadcasted_iota(jnp.int32, (256, 1024), 0)
    c_id = lax.broadcasted_iota(jnp.int32, (256, 1024), 1)
    spread[...] = jnp.where(c_id == 2 * k_id + (c_id // 512) * 513, 1.0, 0.0).astype(BF)
    acc[...] = jnp.zeros_like(acc)

    def settle():
        for cp in small:
            cp.wait()

    group_barrier(z, x, settle)
    yx = lax.rem(x + 2, 4)
    cx = x + 1 - 2 * lax.rem(x, 2)
    cyx = lax.rem(cx + 2, 4)
    near = by_distance(z)

    sent = []
    mine = z * 4 + x
    places = [(z, yx)] + [(zt, xt) for zt in near for xt in (x, yx)]

    def o_send(src, s, zt, xt):
        cp = remote(src, obuf.at[s], ssem_o.at[len(sent)], rsem_o.at[s], zt, xt)
        cp.start()
        sent.append(cp)

    def o_arrived(zt, xt):
        s = zt * 4 + xt
        remote(obuf.at[s], obuf.at[s], ssem_o.at[0], rsem_o.at[s], z, x).wait_recv()

    for zt, xt in places:
        o_send(o_ref.at[zt], mine, zt, xt)
    o_send(o_ref.at[z], mine, z, cx)
    obuf[mine] = o_ref[z]
    for zt, xt in places:
        o_arrived(zt, xt)
        o_send(obuf.at[zt * 4 + xt], zt * 4 + xt, z, cx)
    for zt in (z, *near):
        o_arrived(zt, cx)
        o_arrived(zt, cyx)
    for h in range(8):
        olhs[:, h * 128:(h + 1) * 128] = obuf[:, h].reshape(128, 128)

    loads[0].wait()

    def block(zt):
        return pl.ds(pl.multiple_of(zt * 256, 256), 256)

    for n in range(4):
        lanes = slice(n * 256, (n + 1) * 256)
        low[:, lanes] = jnp.dot(olhs[...], wo[:, lanes], preferred_element_type=F32)
    for i, zt in enumerate(near):
        part[zt] = low[:, block(zt)].astype(BF)
        cp = remote(part.at[zt], recv.at[z], ssem_p.at[i], rsem_p.at[z], zt, x)
        cp.start()
        sent.append(cp)
    total = low[:, block(z)]
    for zt in near:
        remote(recv.at[zt], recv.at[zt], ssem_p.at[0], rsem_p.at[zt], z, x).wait_recv()
        total += recv[zt].astype(F32)
    own = x * 4 + z
    hb[own] = (h_ref[...].astype(F32) + total).astype(BF)
    share_sums(hb[own], stat, ssem_s, rsem_s, z, x)

    def ready():
        scale[...] = scale_of(stat, ssem_s, rsem_s, z, x, 4096)
        for j in range(tiles):
            loads[1 + j].wait()

    def consume(*pair):
        u = jnp.concatenate([normed(hb, gain, g, scale[...]) for g in pair], axis=0)
        wide = jnp.dot(u, spread[...], preferred_element_type=F32).astype(BF)
        rows, width = hb.shape[1], wide.shape[1] // 2
        lhs = [jnp.concatenate([wide[i * rows:(i + 1) * rows, :width], wide[i * rows:(i + 1) * rows, width:]], axis=0)
               for i in range(len(pair))]
        lhs = jnp.concatenate(lhs, axis=1)
        for j in range(0, tiles, 2):
            width = min(2, tiles - j)
            w = jnp.concatenate([
                jnp.concatenate([wg[j + i, pl.ds(pl.multiple_of(g * 512, 512), 512), :] for i in range(width)], axis=1)
                for g in pair], axis=0)
            acc[:, j * 128:(j + width) * 128] += jnp.dot(lhs, w, preferred_element_type=F32)

    sent += gather(hb, lambda zt, xt: xt * 4 + zt, lambda zt: hb.at[own], ssem_h, rsem_h, z, x, ready, consume)
    halves, half = mbuf.shape[0], mbuf.shape[2]

    def m_send(f, xt, target, i):
        cp = remote(mbuf.at[f, xt], mbuf.at[f, xt], ssem_m.at[f, i], rsem_m.at[f, xt], z, target)
        cp.start()
        sent.append(cp)

    def m_arrived(f, xt):
        remote(mbuf.at[f, xt], mbuf.at[f, xt], ssem_m.at[f, 0], rsem_m.at[f, xt], z, x).wait_recv()

    for f in range(halves):
        gate = acc[f * half:(f + 1) * half, :].astype(BF).astype(F32)
        up = acc[128 + f * half:128 + (f + 1) * half, :].astype(BF).astype(F32)
        mbuf[f, x] = (jax.nn.silu(gate) * up).astype(BF)
        m_send(f, x, yx, 0)
        m_send(f, x, cx, 1)
    loads[1 + tiles].wait()

    width = mbuf.shape[3]

    def down(lhs, xt, lanes):
        return jnp.dot(lhs, wd[pl.ds(pl.multiple_of(xt * width, 128), width), lanes], preferred_element_type=F32)

    for xt in (x, cx):
        if xt is cx:
            for f in range(halves):
                m_arrived(f, cx)
        lhs = jnp.concatenate([mbuf[f, xt] for f in range(halves)], axis=0)
        for n in range(4):
            lanes = slice(n * 256, (n + 1) * 256)
            new = down(lhs, xt, lanes)
            low[:, lanes] = new if xt is x else low[:, lanes] + new

    for f in range(halves):
        rows = slice(f * half, (f + 1) * half)
        m_arrived(f, yx)
        m_send(f, yx, cx, 2)
        for n in range(4):
            lanes = slice(n * 256, (n + 1) * 256)
            low[rows, lanes] += down(mbuf[f, yx], yx, lanes)
        m_arrived(f, cyx)

        for n in range(4):
            lanes = slice(n * 256, (n + 1) * 256)
            low[rows, lanes] += down(mbuf[f, cyx], cyx, lanes)
        for i, zt in enumerate(near):
            part2[f, zt] = low[rows, block(zt)].astype(BF)
            cp = remote(part2.at[f, zt], recv2.at[f, z], ssem_q.at[f, i], rsem_q.at[f, z], zt, x)
            cp.start()
            sent.append(cp)
    for f in range(halves):
        rows = slice(f * half, (f + 1) * half)
        total = low[rows, block(z)]
        for zt in near:
            remote(recv2.at[f, zt], recv2.at[f, zt], ssem_q.at[f, 0], rsem_q.at[f, zt], z, x).wait_recv()
            total += recv2[f, zt].astype(F32)
        out_ref[rows, :] = (hb[own, rows, :].astype(F32) + total).astype(BF)
    for cp in sent:
        cp.wait_send()


def solution(mesh):
    hidden_spec = P('replica', ('x', 'yz'))
    batch_axes = ('replica', 'yz', 'x')
    cache_spec = P(None, batch_axes, None, None)
    vmem = pl.BlockSpec(memory_space=pltpu.VMEM)
    smem = pl.BlockSpec(memory_space=pltpu.SMEM)
    hbm = pl.BlockSpec(memory_space=pltpu.HBM)
    dma, sd = pltpu.SemaphoreType.DMA, jax.ShapeDtypeStruct

    def layer(hidden, seq_lens, attn_gain, mlp_gain, w_qkv, w_out, w_gate_up, w_down, k_cache, v_cache):
        w_qkv_t = jnp.swapaxes(w_qkv, 1, 2)
        z_rows = pl.pallas_call(
            qkv_kernel,
            out_shape=sd((16, 8, 384), BF),
            in_specs=[hbm, hbm, hbm],
            out_specs=vmem,
            scratch_shapes=[pltpu.VMEM((128, 256), BF), pltpu.VMEM((1, 4096), BF), pltpu.VMEM((16, 128, 256), BF), pltpu.VMEM((384, 4096), BF), pltpu.VMEM((128, 384), F32),
                            pltpu.VMEM((128, 1), F32), pltpu.VMEM((16, 1, 128), F32),
                            pltpu.VMEM((16, 8, 384), BF), pltpu.VMEM((16, 8, 384), BF),
                            dma((5,)), dma((15,)), dma((16,)), dma((16,)), dma((16,)), dma((16,)), dma((16,))],
            compiler_params=pltpu.CompilerParams(collective_id=0, has_side_effects=True, vmem_limit_bytes=46 * MIB),
            cost_estimate=pl.CostEstimate(flops=30_000_000_000, bytes_accessed=20_000_000, transcendentals=0),
            name="qkv",
        )(hidden, attn_gain, w_qkv_t)
        rows, positions, hd = k_cache.shape[1:]
        o, k_out, v_out = pl.pallas_call(
            attn_kernel,
            out_shape=(sd((4, 8, rows, hd), BF), sd(k_cache.shape, BF), sd(v_cache.shape, BF)),
            in_specs=[smem, vmem, vmem, vmem],
            out_specs=(vmem, hbm, hbm),
            scratch_shapes=[pltpu.VMEM((rows, 34, hd), F32), pltpu.VMEM((rows, 32, hd), F32),
                            pltpu.VMEM((2, rows, 16, hd), BF), dma((2, rows)), dma((2, rows))],
            compiler_params=pltpu.CompilerParams(vmem_limit_bytes=28 * MIB),
            name="attend",
        )(seq_lens, z_rows, k_cache, v_cache)
        hidden = pl.pallas_call(
            mlp_kernel,
            out_shape=sd(hidden.shape, BF),
            in_specs=[hbm] * 6,
            out_specs=vmem,
            scratch_shapes=[pltpu.VMEM((4, 8, 8, 128), BF), pltpu.VMEM((128, 256), BF), pltpu.VMEM((1, 4096), BF),
                            pltpu.VMEM((1024, 1024), BF), pltpu.VMEM((7, 8192, 128), BF), pltpu.VMEM((3584, 1024), BF),
                            pltpu.VMEM((256, 1024), BF), pltpu.VMEM((16, 8, 8, 128), BF), pltpu.VMEM((128, 1024), BF),
                            pltpu.VMEM((4, 128, 256), BF), pltpu.VMEM((4, 128, 256), BF), pltpu.VMEM((16, 128, 256), BF),
                            pltpu.VMEM((256, 896), F32), pltpu.VMEM((128, 1), F32), pltpu.VMEM((16, 1, 128), F32),
                            pltpu.VMEM((2, 4, 64, 896), BF), pltpu.VMEM((128, 1024), F32),
                            pltpu.VMEM((2, 4, 64, 256), BF), pltpu.VMEM((2, 4, 64, 256), BF),
                            dma((12,)), dma((16,)), dma((16,)), dma((15,)), dma((16,)), dma((3,)), dma((4,)), dma((15,)), dma((16,)),
                            dma((2, 3)), dma((2, 4)), dma((2, 3)), dma((2, 4))],
            compiler_params=pltpu.CompilerParams(collective_id=1, has_side_effects=True, vmem_limit_bytes=48 * MIB),
            name="mlp",
        )(o, hidden, mlp_gain, w_out, w_gate_up, w_down)
        return hidden, k_out, v_out

    return jax.shard_map(
        layer,
        mesh=mesh,
        in_specs=(hidden_spec, P(batch_axes), P(), P(), P(None, None, 'yz'), P(None, 'yz', None),
                  P(None, None, None, 'yz'), P(None, 'yz', None), cache_spec, cache_spec),
        out_specs=(hidden_spec, cache_spec, cache_spec),
        check_vma=False)
```

```python
import functools

import jax
import jax.numpy as jnp
from jax import lax
from jax.experimental import pallas as pl
from jax.experimental.pallas import tpu as pltpu
from jax.sharding import PartitionSpec as P

NORM_EPS = 1e-5
MESH = pl.DeviceIdType.MESH
BF = jnp.bfloat16
F32 = jnp.float32
MIB = 1024 * 1024
GROUP = 4
CHUNK = 1024


def at(z, x):
    return {"yz": z, "x": x}


def remote(src, dst, ssem, rsem, z, x):
    return pltpu.make_async_remote_copy(src_ref=src, dst_ref=dst, send_sem=ssem, recv_sem=rsem,
                                        device_id=at(z, x), device_id_type=MESH)


def group_barrier(z, x, between=None):
    sem = pltpu.get_barrier_semaphore()
    me = z * 4 + x

    def body(p, c):
        d = lax.rem(me + p, 16)
        pl.semaphore_signal(sem, inc=1, device_id=at(lax.div(d, 4), lax.rem(d, 4)), device_id_type=MESH)
        return c

    lax.fori_loop(1, 16, body, 0)
    if between is not None:
        between()
    pl.semaphore_wait(sem, 15)


def by_distance(z):
    a, b = lax.div(z, 2), lax.rem(z, 2)
    first = lax.div(z + 3, 4)
    n1 = first * (z - 1) + (1 - first)
    n2 = 2 + a * (1 - 2 * b)
    return n1, n2, 6 - z - n1 - n2


def gather(buf, slot, src, ssem, rsem, z, x, ready, consume):
    yx = lax.rem(x + 2, 4)
    cx = x + 1 - 2 * lax.rem(x, 2)
    cyx = lax.rem(cx + 2, 4)
    n1, n2 = 1 + lax.rem(z, 2), 3 * (1 - lax.div(z, 2))
    n3 = 6 - z - n1 - n2
    end = 1 - lax.div(z * (3 - z), 2)
    me = slot(z, x)
    started = []

    def send(src, s, zt, xt):
        cp = remote(src, buf.at[s], ssem.at[len(started)], rsem.at[s], zt, xt)
        cp.start()
        started.append(cp)

    def arrived(s):
        remote(buf.at[s], buf.at[s], ssem.at[0], rsem.at[s], z, x).wait_recv()

    def pass_on(zt, xt, *targets):
        s = slot(zt, xt)
        arrived(s)
        for t in targets:
            send(buf.at[s], s, z, t)

    def work(first, second, *late):
        for zt, xt in late:
            arrived(slot(zt, xt))
        consume(slot(*first), slot(*second))

    send(src, me, z, yx)
    send(src, me, end * n2 + (1 - end) * n1, x)
    send(src, me, n3, x)
    third = slot(end * z + (1 - end) * n1, x)
    third = remote(buf.at[third], buf.at[third], ssem.at[len(started)], rsem.at[third], end * n1 + (1 - end) * n3, x)
    started.append(third)
    pl.when(end == 1)(third.start)
    send(src, me, z, cx)
    pass_on(z, yx, cx)
    arrived(slot(n1, x))
    pl.when(end == 0)(third.start)
    for t in (yx, cx):
        send(buf.at[slot(n1, x)], slot(n1, x), z, t)
    ready()
    work((z, x), (z, yx))
    pass_on(n2, x, yx, cx)
    work((n1, x), (z, cx), (z, cx))
    pass_on(n3, x, yx, cx)
    work((n2, x), (z, cyx), (z, cyx))
    pass_on(n1, yx, cx)
    work((n3, x), (n1, cx), (n1, cx))
    pass_on(n2, yx, cx)
    work((n1, yx), (n2, cx), (n2, cx))
    work((n2, yx), (n3, cx), (n3, cx))
    pass_on(n3, yx, cx)
    work((n3, yx), (n1, cyx), (n1, cyx))
    work((n2, cyx), (n3, cyx), (n2, cyx), (n3, cyx))
    return started


def share_sums(h, stat, ssem, rsem, z, x):
    me = z * 4 + x
    rows = h.shape[0]
    hf = h.astype(F32)
    sums = jnp.broadcast_to(jnp.sum(hf * hf, axis=1, keepdims=True), (rows, 128))
    stat[me] = jnp.transpose(sums)[0:1, :]

    def peer(p):
        d = lax.rem(me + p, 16)
        return remote(stat.at[me], stat.at[me], ssem.at[p], rsem.at[me], lax.div(d, 4), lax.rem(d, 4))

    def start(p, c):
        peer(p).start()
        return c

    lax.fori_loop(1, 16, start, 0)


def scale_of(stat, ssem, rsem, z, x, width):
    me = z * 4 + x

    def finish(p, c):
        remote(stat.at[me], stat.at[me], ssem.at[p], rsem.at[me], z, x).wait_send()
        d = lax.rem(me + p, 16)
        remote(stat.at[d], stat.at[d], ssem.at[0], rsem.at[d], z, x).wait_recv()
        return c

    lax.fori_loop(1, 16, finish, 0)
    tot = functools.reduce(lambda u, v: u + v, [stat[i] for i in range(16)])
    r = lax.rsqrt(tot / width + NORM_EPS)
    return jnp.transpose(jnp.broadcast_to(r, (128, 128)))[:, 0:1]


def normed(hb, gain, g, r):
    w = hb.shape[2]
    return (hb[g].astype(F32) * r * gain[:, pl.ds(pl.multiple_of(g * w, w), w)].astype(F32)).astype(BF)


def qkv_kernel(h_hbm, gain_hbm, w_hbm, out_ref, h_ref, gain, hb, wbuf, acc, scale, stat, zloc, zbuf,
               wsem, ssem, rsem, ssem_s, rsem_s, ssem2, rsem2):
    z, x = lax.axis_index("yz"), lax.axis_index("x")
    me = z * 4 + x
    parts = [
        pltpu.make_async_copy(w_hbm.at[0, pl.ds(pl.multiple_of(x * 256, 256), 256), :], wbuf.at[pl.ds(0, 256), :], wsem.at[0]),
        pltpu.make_async_copy(w_hbm.at[0, pl.ds(1024, 64), :], wbuf.at[pl.ds(256, 64), :], wsem.at[1]),
        pltpu.make_async_copy(w_hbm.at[0, pl.ds(1024, 64), :], wbuf.at[pl.ds(320, 64), :], wsem.at[2]),
        pltpu.make_async_copy(gain_hbm, gain, wsem.at[3]),
    ]
    mine = pltpu.make_async_copy(h_hbm, h_ref, wsem.at[4])
    mine.start()
    for cp in parts:
        cp.start()
    acc[...] = jnp.zeros_like(acc)
    group_barrier(z, x, mine.wait)
    share_sums(h_ref[...], stat, ssem_s, rsem_s, z, x)
    hb[x * 4 + z] = h_ref[...]

    def ready():
        scale[...] = scale_of(stat, ssem_s, rsem_s, z, x, 4096)
        for cp in parts:
            cp.wait()

    def consume(*pair):
        u = jnp.concatenate([normed(hb, gain, g, scale[...]) for g in pair], axis=1)
        w = jnp.concatenate([wbuf[:, pl.ds(pl.multiple_of(g * 256, 256), 256)] for g in pair], axis=1)
        acc[...] += lax.dot_general(u, w, (((1,), (1,)), ((), ())), preferred_element_type=F32)

    sent = gather(hb, lambda zt, xt: xt * 4 + zt, h_ref, ssem, rsem, z, x, ready, consume)
    for d in range(16):
        zloc[d] = acc[d * 8:(d + 1) * 8, :].astype(BF)

    def peer(p):
        d = lax.rem(me + p, 16)
        return remote(zloc.at[d], zbuf.at[me], ssem2.at[p], rsem2.at[me], lax.div(d, 4), lax.rem(d, 4))

    def start(p, c):
        peer(p).start()
        return c

    def finish(p, c):
        peer(p).wait_send()
        d = lax.rem(me + p, 16)
        remote(zbuf.at[d], zbuf.at[d], ssem2.at[0], rsem2.at[d], z, x).wait_recv()
        return c

    lax.fori_loop(1, 16, start, 0)
    zbuf[me] = zloc[me]
    for cp in sent:
        cp.wait_send()
    lax.fori_loop(1, 16, finish, 0)
    out_ref[...] = zbuf[...]


def attn_kernel(len_ref, z_ref, k_ref, v_ref, o_ref, ko_hbm, vo_hbm, zrow, orow, tiles, qrow, score, osem, tsem):
    rows, positions, hd = k_ref.shape[1:]

    def store(b, which):
        src, dst = ((k_ref, ko_hbm), (v_ref, vo_hbm))[which]
        return pltpu.make_async_copy(src.at[0, b], dst.at[0, b], osem.at[which, b])

    def first(b):
        return pl.multiple_of(lax.div(len_ref[b], 16) * 16, 16)

    def patch(b, which):
        dst = (ko_hbm, vo_hbm)[which]
        return pltpu.make_async_copy(tiles.at[which, b], dst.at[0, b, pl.ds(first(b), 16), :], tsem.at[which, b])

    def start(b, c):
        store(b, 0).start()
        store(b, 1).start()
        return c

    lax.fori_loop(0, rows, start, 0)
    lane = lax.broadcasted_iota(jnp.int32, (rows, hd), 1)
    for pair in range(2):
        base = 17 * pair
        even, odd = 8 * pair, 8 * pair + 4
        mains_e = [z_ref[even + i // 2, :, (i % 2) * hd:(i % 2 + 1) * hd].astype(F32) for i in range(8)]
        mains_o = [pltpu.roll(z_ref[odd + i // 2, :, (i % 2) * hd:(i % 2 + 1) * hd].astype(F32), hd // 2, 1) for i in range(8)]
        tail_e = z_ref[even, :, 2 * hd:3 * hd].astype(F32)
        tail_o = z_ref[odd, :, 2 * hd:3 * hd].astype(F32)
        heads = mains_e + [jnp.where(lane < hd // 2, tail_e, mains_o[0])]
        for i in range(8):
            heads.append(jnp.where(lane < hd // 2, mains_o[i], mains_o[i + 1] if i < 7 else tail_o))
        for i, v in enumerate(heads):
            zrow[:, base + i, :] = v
    heads = zrow.shape[1] - 2
    factor = hd ** -0.5 * 1.4426950408889634

    def updated(ref, b, row, pos):
        lo = first(b)
        tile = ref[0, b, pl.ds(lo, 16), :].astype(F32)
        hit = lax.broadcasted_iota(jnp.int32, (16, hd), 0) == pos - lo
        return jnp.where(hit, row, tile).astype(BF)

    def renew(b, c):
        tiles[0, b] = updated(k_ref, b, zrow[b, heads:heads + 1, :], len_ref[b])
        tiles[1, b] = updated(v_ref, b, zrow[b, heads + 1:heads + 2, :], len_ref[b])
        return c

    lax.fori_loop(0, rows, renew, 0)

    qrow[...] = jnp.zeros_like(qrow)
    lane_row = lax.broadcasted_iota(jnp.int32, (1, GROUP * heads), 1)
    nt = (((1,), (1,)), ((), ()))

    def one(g, c):
        b0 = g * GROUP
        ends = jnp.zeros((1, GROUP * heads), jnp.int32)
        for i in range(GROUP):
            qrow[i * heads:(i + 1) * heads, i * hd:(i + 1) * hd] = zrow[b0 + i, 0:heads, :].astype(BF)
            ends = jnp.where(lax.div(lane_row, heads) == i, len_ref[b0 + i], ends)
        q = qrow[...]
        k_new = jnp.concatenate([jnp.broadcast_to(zrow[b0 + i, heads:heads + 1, :], (8, hd)) for i in range(GROUP)], axis=1)
        s_new = lax.dot_general(k_new.astype(BF), q, nt, preferred_element_type=F32)[0:1, :]
        top = s_new
        for lo in range(0, positions, CHUNK):
            k = jnp.concatenate([k_ref[0, b0 + i, lo:lo + CHUNK, :] for i in range(GROUP)], axis=1)
            s = lax.dot_general(k, q, nt, preferred_element_type=F32)
            ids = lax.broadcasted_iota(jnp.int32, s.shape, 0) + lo
            s = jnp.where(ids < ends, s, -1e30)
            score[lo:lo + CHUNK, :] = s
            top = jnp.maximum(top, jnp.max(s, axis=0, keepdims=True))
        e_new = jnp.exp2((s_new - top) * factor)
        total = e_new
        for lo in range(0, positions, CHUNK):
            e = jnp.exp2((score[lo:lo + CHUNK, :] - top) * factor)
            score[lo:lo + CHUNK, :] = e
            total += jnp.sum(e, axis=0, keepdims=True)
        inv = 1.0 / total
        p_new = jnp.transpose(jnp.broadcast_to((e_new * inv).astype(BF).astype(F32), (GROUP * heads, GROUP * heads)))
        outs = [p_new[i * heads:(i + 1) * heads, 0:1] * zrow[b0 + i, heads + 1:heads + 2, :] for i in range(GROUP)]
        for lo in range(0, positions, CHUNK):
            p = jnp.transpose((score[lo:lo + CHUNK, :] * inv).astype(BF))
            for i in range(GROUP):
                outs[i] += jnp.dot(p[i * heads:(i + 1) * heads, :], v_ref[0, b0 + i, lo:lo + CHUNK, :], preferred_element_type=F32)
        for i in range(GROUP):
            orow[b0 + i] = outs[i]
        return c

    def fix(b):
        for which in range(2):
            store(b, which).wait()
            patch(b, which).start()

    def patches(b, c):
        fix(b)
        return c

    lax.fori_loop(0, rows // GROUP, one, 0)
    lax.fori_loop(0, rows, patches, 0)
    for h in range(heads):
        o_ref[h // 8, h % 8] = orow[:, h, :].astype(BF)

    def finish(b, c):
        for which in range(2):
            patch(b, which).wait()
        return c

    lax.fori_loop(0, rows, finish, 0)


def mlp_kernel(o_hbm, h_hbm, gain_hbm, wo_hbm, wg_hbm, wd_hbm, out_ref,
               o_ref, h_ref, gain, wo, wg, wd, spread, obuf, olhs, part, recv, hb, acc, scale, stat, mbuf, low, part2, recv2,
               wsem, ssem_s, rsem_s, ssem_o, rsem_o, ssem_p, rsem_p, ssem_h, rsem_h, ssem_m, rsem_m, ssem_q, rsem_q):
    z, x = lax.axis_index("yz"), lax.axis_index("x")
    cols = pl.ds(pl.multiple_of(x * 1024, 1024), 1024)
    tiles = wg.shape[0]
    depth = wg.shape[1]
    flat = wg_hbm.at[0].reshape(depth, wg_hbm.shape[3])
    small = [pltpu.make_async_copy(o_hbm, o_ref, wsem.at[2 + tiles]), pltpu.make_async_copy(h_hbm, h_ref, wsem.at[3 + tiles]),
             pltpu.make_async_copy(gain_hbm, gain, wsem.at[4 + tiles])]
    for cp in small:
        cp.start()
    loads = [pltpu.make_async_copy(wo_hbm.at[0, :, cols], wo, wsem.at[0])]
    for j in range(tiles):
        lanes = pl.ds(pl.multiple_of((x * tiles + j) * 128, 128), 128)
        loads.append(pltpu.make_async_copy(flat.at[:, lanes], wg.at[j], wsem.at[1 + j]))
    loads.append(pltpu.make_async_copy(wd_hbm.at[0, :, cols], wd, wsem.at[1 + tiles]))
    for cp in loads:
        cp.start()
    k_id = lax.broadcasted_iota(jnp.int32, (256, 1024), 0)
    c_id = lax.broadcasted_iota(jnp.int32, (256, 1024), 1)
    spread[...] = jnp.where(c_id == 2 * k_id + (c_id // 512) * 513, 1.0, 0.0).astype(BF)
    acc[...] = jnp.zeros_like(acc)

    def settle():
        for cp in small:
            cp.wait()

    group_barrier(z, x, settle)
    yx = lax.rem(x + 2, 4)
    cx = x + 1 - 2 * lax.rem(x, 2)
    cyx = lax.rem(cx + 2, 4)
    near = by_distance(z)

    sent = []
    mine = z * 4 + x
    places = [(z, yx)] + [(zt, xt) for zt in near for xt in (x, yx)]

    def o_send(src, s, zt, xt):
        cp = remote(src, obuf.at[s], ssem_o.at[len(sent)], rsem_o.at[s], zt, xt)
        cp.start()
        sent.append(cp)

    def o_arrived(zt, xt):
        s = zt * 4 + xt
        remote(obuf.at[s], obuf.at[s], ssem_o.at[0], rsem_o.at[s], z, x).wait_recv()

    for zt, xt in places:
        o_send(o_ref.at[zt], mine, zt, xt)
    o_send(o_ref.at[z], mine, z, cx)
    obuf[mine] = o_ref[z]
    for zt, xt in places:
        o_arrived(zt, xt)
        o_send(obuf.at[zt * 4 + xt], zt * 4 + xt, z, cx)
    for zt in (z, *near):
        o_arrived(zt, cx)
        o_arrived(zt, cyx)
    for h in range(8):
        olhs[:, h * 128:(h + 1) * 128] = obuf[:, h].reshape(128, 128)

    loads[0].wait()

    def block(zt):
        return pl.ds(pl.multiple_of(zt * 256, 256), 256)

    for n in range(4):
        lanes = slice(n * 256, (n + 1) * 256)
        low[:, lanes] = jnp.dot(olhs[...], wo[:, lanes], preferred_element_type=F32)
    for i, zt in enumerate(near):
        part[zt] = low[:, block(zt)].astype(BF)
        cp = remote(part.at[zt], recv.at[z], ssem_p.at[i], rsem_p.at[z], zt, x)
        cp.start()
        sent.append(cp)
    total = low[:, block(z)]
    for zt in near:
        remote(recv.at[zt], recv.at[zt], ssem_p.at[0], rsem_p.at[zt], z, x).wait_recv()
        total += recv[zt].astype(F32)
    own = x * 4 + z
    hb[own] = (h_ref[...].astype(F32) + total).astype(BF)
    share_sums(hb[own], stat, ssem_s, rsem_s, z, x)

    def ready():
        scale[...] = scale_of(stat, ssem_s, rsem_s, z, x, 4096)
        for j in range(tiles):
            loads[1 + j].wait()

    def consume(*pair):
        u = jnp.concatenate([normed(hb, gain, g, scale[...]) for g in pair], axis=0)
        wide = jnp.dot(u, spread[...], preferred_element_type=F32).astype(BF)
        rows, width = hb.shape[1], wide.shape[1] // 2
        lhs = [jnp.concatenate([wide[i * rows:(i + 1) * rows, :width], wide[i * rows:(i + 1) * rows, width:]], axis=0)
               for i in range(len(pair))]
        lhs = jnp.concatenate(lhs, axis=1)
        for j in range(0, tiles, 2):
            width = min(2, tiles - j)
            w = jnp.concatenate([
                jnp.concatenate([wg[j + i, pl.ds(pl.multiple_of(g * 512, 512), 512), :] for i in range(width)], axis=1)
                for g in pair], axis=0)
            acc[:, j * 128:(j + width) * 128] += jnp.dot(lhs, w, preferred_element_type=F32)

    sent += gather(hb, lambda zt, xt: xt * 4 + zt, hb.at[own], ssem_h, rsem_h, z, x, ready, consume)
    halves, half = mbuf.shape[0], mbuf.shape[2]

    def m_send(f, xt, target, i):
        cp = remote(mbuf.at[f, xt], mbuf.at[f, xt], ssem_m.at[f, i], rsem_m.at[f, xt], z, target)
        cp.start()
        sent.append(cp)

    def m_arrived(f, xt):
        remote(mbuf.at[f, xt], mbuf.at[f, xt], ssem_m.at[f, 0], rsem_m.at[f, xt], z, x).wait_recv()

    for f in range(halves):
        gate = acc[f * half:(f + 1) * half, :].astype(BF).astype(F32)
        up = acc[128 + f * half:128 + (f + 1) * half, :].astype(BF).astype(F32)
        mbuf[f, x] = (jax.nn.silu(gate) * up).astype(BF)
        m_send(f, x, yx, 0)
        m_send(f, x, cx, 1)
    loads[1 + tiles].wait()

    width = mbuf.shape[3]

    def down(lhs, xt, lanes):
        return jnp.dot(lhs, wd[pl.ds(pl.multiple_of(xt * width, 128), width), lanes], preferred_element_type=F32)

    for xt in (x, cx):
        if xt is cx:
            for f in range(halves):
                m_arrived(f, cx)
        lhs = jnp.concatenate([mbuf[f, xt] for f in range(halves)], axis=0)
        for n in range(4):
            lanes = slice(n * 256, (n + 1) * 256)
            new = down(lhs, xt, lanes)
            low[:, lanes] = new if xt is x else low[:, lanes] + new

    for f in range(halves):
        rows = slice(f * half, (f + 1) * half)
        m_arrived(f, yx)
        m_send(f, yx, cx, 2)
        for n in range(4):
            lanes = slice(n * 256, (n + 1) * 256)
            low[rows, lanes] += down(mbuf[f, yx], yx, lanes)
        m_arrived(f, cyx)

        for n in range(4):
            lanes = slice(n * 256, (n + 1) * 256)
            low[rows, lanes] += down(mbuf[f, cyx], cyx, lanes)
        for i, zt in enumerate(near):
            part2[f, zt] = low[rows, block(zt)].astype(BF)
            cp = remote(part2.at[f, zt], recv2.at[f, z], ssem_q.at[f, i], rsem_q.at[f, z], zt, x)
            cp.start()
            sent.append(cp)
    for f in range(halves):
        rows = slice(f * half, (f + 1) * half)
        total = low[rows, block(z)]
        for zt in near:
            remote(recv2.at[f, zt], recv2.at[f, zt], ssem_q.at[f, 0], rsem_q.at[f, zt], z, x).wait_recv()
            total += recv2[f, zt].astype(F32)
        out_ref[rows, :] = (hb[own, rows, :].astype(F32) + total).astype(BF)
    for cp in sent:
        cp.wait_send()


def solution(mesh):
    hidden_spec = P('replica', ('x', 'yz'))
    batch_axes = ('replica', 'yz', 'x')
    cache_spec = P(None, batch_axes, None, None)
    vmem = pl.BlockSpec(memory_space=pltpu.VMEM)
    smem = pl.BlockSpec(memory_space=pltpu.SMEM)
    hbm = pl.BlockSpec(memory_space=pltpu.HBM)
    dma, sd = pltpu.SemaphoreType.DMA, jax.ShapeDtypeStruct

    def layer(hidden, seq_lens, attn_gain, mlp_gain, w_qkv, w_out, w_gate_up, w_down, k_cache, v_cache):
        w_qkv_t = jnp.swapaxes(w_qkv, 1, 2)
        z_rows = pl.pallas_call(
            qkv_kernel,
            out_shape=sd((16, 8, 384), BF),
            in_specs=[hbm, hbm, hbm],
            out_specs=vmem,
            scratch_shapes=[pltpu.VMEM((128, 256), BF), pltpu.VMEM((1, 4096), BF), pltpu.VMEM((16, 128, 256), BF), pltpu.VMEM((384, 4096), BF), pltpu.VMEM((128, 384), F32),
                            pltpu.VMEM((128, 1), F32), pltpu.VMEM((16, 1, 128), F32),
                            pltpu.VMEM((16, 8, 384), BF), pltpu.VMEM((16, 8, 384), BF),
                            dma((5,)), dma((15,)), dma((16,)), dma((16,)), dma((16,)), dma((16,)), dma((16,))],
            compiler_params=pltpu.CompilerParams(collective_id=0, has_side_effects=True, vmem_limit_bytes=46 * MIB),
            cost_estimate=pl.CostEstimate(flops=30_000_000_000, bytes_accessed=20_000_000, transcendentals=0),
            name="qkv",
        )(pltpu.with_memory_space_constraint(hidden, pltpu.HBM), pltpu.with_memory_space_constraint(attn_gain, pltpu.HBM), w_qkv_t)
        rows, positions, hd = k_cache.shape[1:]
        o, k_out, v_out = pl.pallas_call(
            attn_kernel,
            out_shape=(sd((4, 8, rows, hd), BF), sd(k_cache.shape, BF), sd(v_cache.shape, BF)),
            in_specs=[smem, vmem, vmem, vmem],
            out_specs=(vmem, hbm, hbm),
            scratch_shapes=[pltpu.VMEM((rows, 34, hd), F32), pltpu.VMEM((rows, 32, hd), F32),
                            pltpu.VMEM((2, rows, 16, hd), BF), pltpu.VMEM((GROUP * 32, GROUP * hd), BF),
                            pltpu.VMEM((positions, GROUP * 32), F32), dma((2, rows)), dma((2, rows))],
            compiler_params=pltpu.CompilerParams(vmem_limit_bytes=28 * MIB),
            name="attend",
        )(seq_lens, z_rows, k_cache, v_cache)
        hidden = pl.pallas_call(
            mlp_kernel,
            out_shape=sd(hidden.shape, BF),
            in_specs=[hbm] * 6,
            out_specs=vmem,
            scratch_shapes=[pltpu.VMEM((4, 8, 8, 128), BF), pltpu.VMEM((128, 256), BF), pltpu.VMEM((1, 4096), BF),
                            pltpu.VMEM((1024, 1024), BF), pltpu.VMEM((7, 8192, 128), BF), pltpu.VMEM((3584, 1024), BF),
                            pltpu.VMEM((256, 1024), BF), pltpu.VMEM((16, 8, 8, 128), BF), pltpu.VMEM((128, 1024), BF),
                            pltpu.VMEM((4, 128, 256), BF), pltpu.VMEM((4, 128, 256), BF), pltpu.VMEM((16, 128, 256), BF),
                            pltpu.VMEM((256, 896), F32), pltpu.VMEM((128, 1), F32), pltpu.VMEM((16, 1, 128), F32),
                            pltpu.VMEM((2, 4, 64, 896), BF), pltpu.VMEM((128, 1024), F32),
                            pltpu.VMEM((2, 4, 64, 256), BF), pltpu.VMEM((2, 4, 64, 256), BF),
                            dma((12,)), dma((16,)), dma((16,)), dma((15,)), dma((16,)), dma((3,)), dma((4,)), dma((15,)), dma((16,)),
                            dma((2, 3)), dma((2, 4)), dma((2, 3)), dma((2, 4))],
            compiler_params=pltpu.CompilerParams(collective_id=1, has_side_effects=True, vmem_limit_bytes=48 * MIB),
            name="mlp",
        )(o, hidden, mlp_gain, w_out, w_gate_up, w_down)
        return hidden, k_out, v_out

    return jax.shard_map(
        layer,
        mesh=mesh,
        in_specs=(hidden_spec, P(batch_axes), P(), P(), P(None, None, 'yz'), P(None, 'yz', None),
                  P(None, None, None, 'yz'), P(None, 'yz', None), cache_spec, cache_spec),
        out_specs=(hidden_spec, cache_spec, cache_spec),
        check_vma=False)
```

```python
import functools

import jax
import jax.numpy as jnp
from jax import lax
from jax.experimental import pallas as pl
from jax.experimental.pallas import tpu as pltpu
from jax.sharding import PartitionSpec as P

NORM_EPS = 1e-5
MESH = pl.DeviceIdType.MESH
BF = jnp.bfloat16
F32 = jnp.float32
MIB = 1024 * 1024
GROUP = 4
CHUNK = 1024


def at(z, x):
    return {"yz": z, "x": x}


def remote(src, dst, ssem, rsem, z, x):
    return pltpu.make_async_remote_copy(src_ref=src, dst_ref=dst, send_sem=ssem, recv_sem=rsem,
                                        device_id=at(z, x), device_id_type=MESH)


def group_barrier(z, x, between=None):
    sem = pltpu.get_barrier_semaphore()
    me = z * 4 + x

    def body(p, c):
        d = lax.rem(me + p, 16)
        pl.semaphore_signal(sem, inc=1, device_id=at(lax.div(d, 4), lax.rem(d, 4)), device_id_type=MESH)
        return c

    lax.fori_loop(1, 16, body, 0)
    if between is not None:
        between()
    pl.semaphore_wait(sem, 15)


def by_distance(z):
    a, b = lax.div(z, 2), lax.rem(z, 2)
    first = lax.div(z + 3, 4)
    n1 = first * (z - 1) + (1 - first)
    n2 = 2 + a * (1 - 2 * b)
    return n1, n2, 6 - z - n1 - n2


def gather(buf, slot, src, ssem, rsem, z, x, ready, consume):
    yx = lax.rem(x + 2, 4)
    cx = x + 1 - 2 * lax.rem(x, 2)
    cyx = lax.rem(cx + 2, 4)
    n1, n2 = 1 + lax.rem(z, 2), 3 * (1 - lax.div(z, 2))
    n3 = 6 - z - n1 - n2
    end = 1 - lax.div(z * (3 - z), 2)
    me = slot(z, x)
    started = []

    def send(src, s, zt, xt):
        cp = remote(src, buf.at[s], ssem.at[len(started)], rsem.at[s], zt, xt)
        cp.start()
        started.append(cp)

    def arrived(s):
        remote(buf.at[s], buf.at[s], ssem.at[0], rsem.at[s], z, x).wait_recv()

    def pass_on(zt, xt, *targets):
        s = slot(zt, xt)
        arrived(s)
        for t in targets:
            send(buf.at[s], s, z, t)

    def work(first, second, *late):
        for zt, xt in late:
            arrived(slot(zt, xt))
        consume(slot(*first), slot(*second))

    send(src, me, z, yx)
    send(src, me, end * n2 + (1 - end) * n1, x)
    send(src, me, n3, x)
    third = slot(end * z + (1 - end) * n1, x)
    third = remote(buf.at[third], buf.at[third], ssem.at[len(started)], rsem.at[third], end * n1 + (1 - end) * n3, x)
    started.append(third)
    pl.when(end == 1)(third.start)
    send(src, me, z, cx)
    pass_on(z, yx, cx)
    arrived(slot(n1, x))
    pl.when(end == 0)(third.start)
    for t in (yx, cx):
        send(buf.at[slot(n1, x)], slot(n1, x), z, t)
    ready()
    work((z, x), (z, yx))
    pass_on(n2, x, yx, cx)
    work((n1, x), (z, cx), (z, cx))
    pass_on(n3, x, yx, cx)
    work((n2, x), (z, cyx), (z, cyx))
    pass_on(n1, yx, cx)
    work((n3, x), (n1, cx), (n1, cx))
    pass_on(n2, yx, cx)
    work((n1, yx), (n2, cx), (n2, cx))
    work((n2, yx), (n3, cx), (n3, cx))
    pass_on(n3, yx, cx)
    work((n3, yx), (n1, cyx), (n1, cyx))
    work((n2, cyx), (n3, cyx), (n2, cyx), (n3, cyx))
    return started


def share_sums(h, stat, ssem, rsem, z, x):
    me = z * 4 + x
    rows = h.shape[0]
    hf = h.astype(F32)
    sums = jnp.broadcast_to(jnp.sum(hf * hf, axis=1, keepdims=True), (rows, 128))
    stat[me] = jnp.transpose(sums)[0:1, :]

    def peer(p):
        d = lax.rem(me + p, 16)
        return remote(stat.at[me], stat.at[me], ssem.at[p], rsem.at[me], lax.div(d, 4), lax.rem(d, 4))

    def start(p, c):
        peer(p).start()
        return c

    lax.fori_loop(1, 16, start, 0)


def scale_of(stat, ssem, rsem, z, x, width):
    me = z * 4 + x

    def finish(p, c):
        remote(stat.at[me], stat.at[me], ssem.at[p], rsem.at[me], z, x).wait_send()
        d = lax.rem(me + p, 16)
        remote(stat.at[d], stat.at[d], ssem.at[0], rsem.at[d], z, x).wait_recv()
        return c

    lax.fori_loop(1, 16, finish, 0)
    tot = functools.reduce(lambda u, v: u + v, [stat[i] for i in range(16)])
    r = lax.rsqrt(tot / width + NORM_EPS)
    return jnp.transpose(jnp.broadcast_to(r, (128, 128)))[:, 0:1]


def normed(hb, gain, g, r):
    w = hb.shape[2]
    return (hb[g].astype(F32) * r * gain[:, pl.ds(pl.multiple_of(g * w, w), w)].astype(F32)).astype(BF)


def qkv_kernel(h_hbm, gain_hbm, w_hbm, out_ref, h_ref, gain, hb, wbuf, acc, scale, stat, zloc, zbuf,
               wsem, ssem, rsem, ssem_s, rsem_s, ssem2, rsem2):
    z, x = lax.axis_index("yz"), lax.axis_index("x")
    me = z * 4 + x
    parts = [
        pltpu.make_async_copy(w_hbm.at[0, pl.ds(pl.multiple_of(x * 256, 256), 256), :], wbuf.at[pl.ds(0, 256), :], wsem.at[0]),
        pltpu.make_async_copy(w_hbm.at[0, pl.ds(1024, 64), :], wbuf.at[pl.ds(256, 64), :], wsem.at[1]),
        pltpu.make_async_copy(w_hbm.at[0, pl.ds(1024, 64), :], wbuf.at[pl.ds(320, 64), :], wsem.at[2]),
        pltpu.make_async_copy(gain_hbm, gain, wsem.at[3]),
    ]
    mine = pltpu.make_async_copy(h_hbm, h_ref, wsem.at[4])
    mine.start()
    for cp in parts:
        cp.start()
    acc[...] = jnp.zeros_like(acc)
    group_barrier(z, x, mine.wait)
    share_sums(h_ref[...], stat, ssem_s, rsem_s, z, x)
    hb[x * 4 + z] = h_ref[...]

    def ready():
        scale[...] = scale_of(stat, ssem_s, rsem_s, z, x, 4096)
        for cp in parts:
            cp.wait()

    def consume(*pair):
        u = jnp.concatenate([normed(hb, gain, g, scale[...]) for g in pair], axis=1)
        w = jnp.concatenate([wbuf[:, pl.ds(pl.multiple_of(g * 256, 256), 256)] for g in pair], axis=1)
        acc[...] += lax.dot_general(u, w, (((1,), (1,)), ((), ())), preferred_element_type=F32)

    sent = gather(hb, lambda zt, xt: xt * 4 + zt, h_ref, ssem, rsem, z, x, ready, consume)
    for d in range(16):
        zloc[d] = acc[d * 8:(d + 1) * 8, :].astype(BF)

    def peer(p):
        d = lax.rem(me + p, 16)
        return remote(zloc.at[d], zbuf.at[me], ssem2.at[p], rsem2.at[me], lax.div(d, 4), lax.rem(d, 4))

    def start(p, c):
        peer(p).start()
        return c

    def finish(p, c):
        peer(p).wait_send()
        d = lax.rem(me + p, 16)
        remote(zbuf.at[d], zbuf.at[d], ssem2.at[0], rsem2.at[d], z, x).wait_recv()
        return c

    lax.fori_loop(1, 16, start, 0)
    zbuf[me] = zloc[me]
    for cp in sent:
        cp.wait_send()
    lax.fori_loop(1, 16, finish, 0)
    out_ref[...] = zbuf[...]


def attn_kernel(len_ref, z_ref, k_ref, v_ref, o_ref, ko_hbm, vo_hbm, zrow, orow, tiles, qrow, score, osem, tsem):
    rows, positions, hd = k_ref.shape[1:]

    def store(b, which):
        src, dst = ((k_ref, ko_hbm), (v_ref, vo_hbm))[which]
        return pltpu.make_async_copy(src.at[0, b], dst.at[0, b], osem.at[which, b])

    def first(b):
        return pl.multiple_of(lax.div(len_ref[b], 16) * 16, 16)

    def patch(b, which):
        dst = (ko_hbm, vo_hbm)[which]
        return pltpu.make_async_copy(tiles.at[which, b], dst.at[0, b, pl.ds(first(b), 16), :], tsem.at[which, b])

    def start(b, c):
        store(b, 0).start()
        store(b, 1).start()
        return c

    lax.fori_loop(0, rows, start, 0)
    lane = lax.broadcasted_iota(jnp.int32, (rows, hd), 1)
    for pair in range(2):
        base = 17 * pair
        even, odd = 8 * pair, 8 * pair + 4
        mains_e = [z_ref[even + i // 2, :, (i % 2) * hd:(i % 2 + 1) * hd].astype(F32) for i in range(8)]
        mains_o = [pltpu.roll(z_ref[odd + i // 2, :, (i % 2) * hd:(i % 2 + 1) * hd].astype(F32), hd // 2, 1) for i in range(8)]
        tail_e = z_ref[even, :, 2 * hd:3 * hd].astype(F32)
        tail_o = z_ref[odd, :, 2 * hd:3 * hd].astype(F32)
        heads = mains_e + [jnp.where(lane < hd // 2, tail_e, mains_o[0])]
        for i in range(8):
            heads.append(jnp.where(lane < hd // 2, mains_o[i], mains_o[i + 1] if i < 7 else tail_o))
        for i, v in enumerate(heads):
            zrow[:, base + i, :] = v
    heads = zrow.shape[1] - 2
    factor = hd ** -0.5 * 1.4426950408889634

    def updated(ref, b, row, pos):
        lo = first(b)
        tile = ref[0, b, pl.ds(lo, 16), :].astype(F32)
        hit = lax.broadcasted_iota(jnp.int32, (16, hd), 0) == pos - lo
        return jnp.where(hit, row, tile).astype(BF)

    def renew(b, c):
        tiles[0, b] = updated(k_ref, b, zrow[b, heads:heads + 1, :], len_ref[b])
        tiles[1, b] = updated(v_ref, b, zrow[b, heads + 1:heads + 2, :], len_ref[b])
        return c

    lax.fori_loop(0, rows, renew, 0)

    qrow[...] = jnp.zeros_like(qrow)
    lane_row = lax.broadcasted_iota(jnp.int32, (1, GROUP * heads), 1)
    nt = (((1,), (1,)), ((), ()))

    def one(g, c):
        b0 = g * GROUP
        ends = jnp.zeros((1, GROUP * heads), jnp.int32)
        for i in range(GROUP):
            qrow[i * heads:(i + 1) * heads, i * hd:(i + 1) * hd] = zrow[b0 + i, 0:heads, :].astype(BF)
            ends = jnp.where(lax.div(lane_row, heads) == i, len_ref[b0 + i], ends)
        q = qrow[...]
        k_new = jnp.concatenate([jnp.broadcast_to(zrow[b0 + i, heads:heads + 1, :], (8, hd)) for i in range(GROUP)], axis=1)
        s_new = lax.dot_general(k_new.astype(BF), q, nt, preferred_element_type=F32)[0:1, :]
        top = s_new
        for lo in range(0, positions, CHUNK):
            k = jnp.concatenate([k_ref[0, b0 + i, lo:lo + CHUNK, :] for i in range(GROUP)], axis=1)
            s = lax.dot_general(k, q, nt, preferred_element_type=F32)
            ids = lax.broadcasted_iota(jnp.int32, s.shape, 0) + lo
            s = jnp.where(ids < ends, s, -1e30)
            score[lo:lo + CHUNK, :] = s
            top = jnp.maximum(top, jnp.max(s, axis=0, keepdims=True))
        e_new = jnp.exp2((s_new - top) * factor)
        total = e_new
        for lo in range(0, positions, CHUNK):
            e = jnp.exp2((score[lo:lo + CHUNK, :] - top) * factor)
            score[lo:lo + CHUNK, :] = e
            total += jnp.sum(e, axis=0, keepdims=True)
        inv = 1.0 / total
        p_new = jnp.transpose(jnp.broadcast_to((e_new * inv).astype(BF).astype(F32), (GROUP * heads, GROUP * heads)))
        outs = [p_new[i * heads:(i + 1) * heads, 0:1] * zrow[b0 + i, heads + 1:heads + 2, :] for i in range(GROUP)]
        for lo in range(0, positions, CHUNK):
            p = jnp.transpose((score[lo:lo + CHUNK, :] * inv).astype(BF))
            for i in range(GROUP):
                outs[i] += jnp.dot(p[i * heads:(i + 1) * heads, :], v_ref[0, b0 + i, lo:lo + CHUNK, :], preferred_element_type=F32)
        for i in range(GROUP):
            orow[b0 + i] = outs[i]
        return c

    def fix(b):
        for which in range(2):
            store(b, which).wait()
            patch(b, which).start()

    def patches(b, c):
        fix(b)
        return c

    lax.fori_loop(0, rows // GROUP, one, 0)
    lax.fori_loop(0, rows, patches, 0)
    for h in range(heads):
        o_ref[h // 8, h % 8] = orow[:, h, :].astype(BF)

    def finish(b, c):
        for which in range(2):
            patch(b, which).wait()
        return c

    lax.fori_loop(0, rows, finish, 0)


def mlp_kernel(o_hbm, h_hbm, gain_hbm, wo_hbm, wg_hbm, wd_hbm, out_ref,
               o_ref, h_ref, gain, wo, wg, wd, spread, obuf, olhs, part, recv, hb, acc, scale, stat, mbuf, low, part2, recv2,
               wsem, ssem_s, rsem_s, ssem_o, rsem_o, ssem_p, rsem_p, ssem_h, rsem_h, ssem_m, rsem_m, ssem_q, rsem_q):
    z, x = lax.axis_index("yz"), lax.axis_index("x")
    cols = pl.ds(pl.multiple_of(x * 1024, 1024), 1024)
    tiles = wg.shape[0]
    depth = wg.shape[1]
    flat = wg_hbm.at[0].reshape(depth, wg_hbm.shape[3])
    small = [pltpu.make_async_copy(o_hbm, o_ref, wsem.at[2 + tiles]), pltpu.make_async_copy(h_hbm, h_ref, wsem.at[3 + tiles]),
             pltpu.make_async_copy(gain_hbm, gain, wsem.at[4 + tiles])]
    for cp in small:
        cp.start()
    loads = [pltpu.make_async_copy(wo_hbm.at[0, :, cols], wo, wsem.at[0])]
    for j in range(tiles):
        lanes = pl.ds(pl.multiple_of((x * tiles + j) * 128, 128), 128)
        loads.append(pltpu.make_async_copy(flat.at[:, lanes], wg.at[j], wsem.at[1 + j]))
    loads.append(pltpu.make_async_copy(wd_hbm.at[0, :, cols], wd, wsem.at[1 + tiles]))
    for cp in loads:
        cp.start()
    def settle():
        k_id = lax.broadcasted_iota(jnp.int32, (256, 1024), 0)
        c_id = lax.broadcasted_iota(jnp.int32, (256, 1024), 1)
        spread[...] = jnp.where(c_id == 2 * k_id + (c_id // 512) * 513, 1.0, 0.0).astype(BF)
        acc[...] = jnp.zeros_like(acc)
        for cp in small:
            cp.wait()

    group_barrier(z, x, settle)
    yx = lax.rem(x + 2, 4)
    cx = x + 1 - 2 * lax.rem(x, 2)
    cyx = lax.rem(cx + 2, 4)
    near = by_distance(z)

    sent = []
    mine = z * 4 + x
    places = [(z, yx)] + [(zt, xt) for zt in near for xt in (x, yx)]

    def o_send(src, s, zt, xt):
        cp = remote(src, obuf.at[s], ssem_o.at[len(sent)], rsem_o.at[s], zt, xt)
        cp.start()
        sent.append(cp)

    def o_arrived(zt, xt):
        s = zt * 4 + xt
        remote(obuf.at[s], obuf.at[s], ssem_o.at[0], rsem_o.at[s], z, x).wait_recv()

    for zt, xt in places:
        o_send(o_ref.at[zt], mine, zt, xt)
    o_send(o_ref.at[z], mine, z, cx)
    obuf[mine] = o_ref[z]
    for zt, xt in places:
        o_arrived(zt, xt)
        o_send(obuf.at[zt * 4 + xt], zt * 4 + xt, z, cx)
    for zt in (z, *near):
        o_arrived(zt, cx)
        o_arrived(zt, cyx)
    for h in range(8):
        olhs[:, h * 128:(h + 1) * 128] = obuf[:, h].reshape(128, 128)

    loads[0].wait()

    def block(zt):
        return pl.ds(pl.multiple_of(zt * 256, 256), 256)

    for n in range(4):
        lanes = slice(n * 256, (n + 1) * 256)
        low[:, lanes] = jnp.dot(olhs[...], wo[:, lanes], preferred_element_type=F32)
    for i, zt in enumerate(near):
        part[zt] = low[:, block(zt)].astype(BF)
        cp = remote(part.at[zt], recv.at[z], ssem_p.at[i], rsem_p.at[z], zt, x)
        cp.start()
        sent.append(cp)
    total = low[:, block(z)]
    for zt in near:
        remote(recv.at[zt], recv.at[zt], ssem_p.at[0], rsem_p.at[zt], z, x).wait_recv()
        total += recv[zt].astype(F32)
    own = x * 4 + z
    hb[own] = (h_ref[...].astype(F32) + total).astype(BF)
    share_sums(hb[own], stat, ssem_s, rsem_s, z, x)

    def ready():
        scale[...] = scale_of(stat, ssem_s, rsem_s, z, x, 4096)
        for j in range(tiles):
            loads[1 + j].wait()

    def consume(*pair):
        u = jnp.concatenate([normed(hb, gain, g, scale[...]) for g in pair], axis=0)
        wide = jnp.dot(u, spread[...], preferred_element_type=F32).astype(BF)
        rows, width = hb.shape[1], wide.shape[1] // 2
        lhs = [jnp.concatenate([wide[i * rows:(i + 1) * rows, :width], wide[i * rows:(i + 1) * rows, width:]], axis=0)
               for i in range(len(pair))]
        lhs = jnp.concatenate(lhs, axis=1)
        for j in range(0, tiles, 2):
            width = min(2, tiles - j)
            w = jnp.concatenate([
                jnp.concatenate([wg[j + i, pl.ds(pl.multiple_of(g * 512, 512), 512), :] for i in range(width)], axis=1)
                for g in pair], axis=0)
            acc[:, j * 128:(j + width) * 128] += jnp.dot(lhs, w, preferred_element_type=F32)

    sent += gather(hb, lambda zt, xt: xt * 4 + zt, hb.at[own], ssem_h, rsem_h, z, x, ready, consume)
    pieces, half = mbuf.shape[0], mbuf.shape[2]

    def m_send(f, xt, target, i):
        cp = remote(mbuf.at[f, xt], mbuf.at[f, xt], ssem_m.at[f, i], rsem_m.at[f, xt], z, target)
        cp.start()
        sent.append(cp)

    def m_arrived(f, xt):
        remote(mbuf.at[f, xt], mbuf.at[f, xt], ssem_m.at[f, 0], rsem_m.at[f, xt], z, x).wait_recv()

    for f in range(pieces):
        gate = acc[f * half:(f + 1) * half, :].astype(BF).astype(F32)
        up = acc[128 + f * half:128 + (f + 1) * half, :].astype(BF).astype(F32)
        mbuf[f, x] = (jax.nn.silu(gate) * up).astype(BF)
        m_send(f, x, yx, 0)
        m_send(f, x, cx, 1)
    loads[1 + tiles].wait()

    width = mbuf.shape[3]

    def down(lhs, xt, lanes):
        return jnp.dot(lhs, wd[pl.ds(pl.multiple_of(xt * width, 128), width), lanes], preferred_element_type=F32)

    for xt in (x, cx):
        if xt is cx:
            for f in range(pieces):
                m_arrived(f, cx)
        lhs = jnp.concatenate([mbuf[f, xt] for f in range(pieces)], axis=0)
        for n in range(4):
            lanes = slice(n * 256, (n + 1) * 256)
            new = down(lhs, xt, lanes)
            low[:, lanes] = new if xt is x else low[:, lanes] + new

    def m_pass(f):
        m_arrived(f, yx)
        m_send(f, yx, cx, 2)

    m_pass(0)
    for f in range(pieces):
        rows = slice(f * half, (f + 1) * half)
        if f + 1 < pieces:
            m_pass(f + 1)
        m_arrived(f, cyx)
        for n in range(4):
            lanes = slice(n * 256, (n + 1) * 256)
            low[rows, lanes] += down(mbuf[f, yx], yx, lanes) + down(mbuf[f, cyx], cyx, lanes)
        for i, zt in enumerate(near):
            part2[f, zt] = low[rows, block(zt)].astype(BF)
            cp = remote(part2.at[f, zt], recv2.at[f, z], ssem_q.at[f, i], rsem_q.at[f, z], zt, x)
            cp.start()
            sent.append(cp)
    for f in range(pieces):
        rows = slice(f * half, (f + 1) * half)
        total = low[rows, block(z)]
        for zt in near:
            remote(recv2.at[f, zt], recv2.at[f, zt], ssem_q.at[f, 0], rsem_q.at[f, zt], z, x).wait_recv()
            total += recv2[f, zt].astype(F32)
        out_ref[rows, :] = (hb[own, rows, :].astype(F32) + total).astype(BF)
    for cp in sent:
        cp.wait_send()


def solution(mesh):
    hidden_spec = P('replica', ('x', 'yz'))
    batch_axes = ('replica', 'yz', 'x')
    cache_spec = P(None, batch_axes, None, None)
    vmem = pl.BlockSpec(memory_space=pltpu.VMEM)
    smem = pl.BlockSpec(memory_space=pltpu.SMEM)
    hbm = pl.BlockSpec(memory_space=pltpu.HBM)
    dma, sd = pltpu.SemaphoreType.DMA, jax.ShapeDtypeStruct

    def layer(hidden, seq_lens, attn_gain, mlp_gain, w_qkv, w_out, w_gate_up, w_down, k_cache, v_cache):
        w_qkv_t = jnp.swapaxes(w_qkv, 1, 2)
        z_rows = pl.pallas_call(
            qkv_kernel,
            out_shape=sd((16, 8, 384), BF),
            in_specs=[hbm, hbm, hbm],
            out_specs=vmem,
            scratch_shapes=[pltpu.VMEM((128, 256), BF), pltpu.VMEM((1, 4096), BF), pltpu.VMEM((16, 128, 256), BF), pltpu.VMEM((384, 4096), BF), pltpu.VMEM((128, 384), F32),
                            pltpu.VMEM((128, 1), F32), pltpu.VMEM((16, 1, 128), F32),
                            pltpu.VMEM((16, 8, 384), BF), pltpu.VMEM((16, 8, 384), BF),
                            dma((5,)), dma((15,)), dma((16,)), dma((16,)), dma((16,)), dma((16,)), dma((16,))],
            compiler_params=pltpu.CompilerParams(collective_id=0, has_side_effects=True, vmem_limit_bytes=46 * MIB),
            cost_estimate=pl.CostEstimate(flops=30_000_000_000, bytes_accessed=20_000_000, transcendentals=0),
            name="qkv",
        )(pltpu.with_memory_space_constraint(hidden, pltpu.HBM), pltpu.with_memory_space_constraint(attn_gain, pltpu.HBM), w_qkv_t)
        rows, positions, hd = k_cache.shape[1:]
        o, k_out, v_out = pl.pallas_call(
            attn_kernel,
            out_shape=(sd((4, 8, rows, hd), BF), sd(k_cache.shape, BF), sd(v_cache.shape, BF)),
            in_specs=[smem, vmem, vmem, vmem],
            out_specs=(vmem, hbm, hbm),
            scratch_shapes=[pltpu.VMEM((rows, 34, hd), F32), pltpu.VMEM((rows, 32, hd), F32),
                            pltpu.VMEM((2, rows, 16, hd), BF), pltpu.VMEM((GROUP * 32, GROUP * hd), BF),
                            pltpu.VMEM((positions, GROUP * 32), F32), dma((2, rows)), dma((2, rows))],
            compiler_params=pltpu.CompilerParams(vmem_limit_bytes=28 * MIB),
            name="attend",
        )(seq_lens, z_rows, k_cache, v_cache)
        hidden = pl.pallas_call(
            mlp_kernel,
            out_shape=sd(hidden.shape, BF),
            in_specs=[hbm] * 6,
            out_specs=vmem,
            scratch_shapes=[pltpu.VMEM((4, 8, 8, 128), BF), pltpu.VMEM((128, 256), BF), pltpu.VMEM((1, 4096), BF),
                            pltpu.VMEM((1024, 1024), BF), pltpu.VMEM((7, 8192, 128), BF), pltpu.VMEM((3584, 1024), BF),
                            pltpu.VMEM((256, 1024), BF), pltpu.VMEM((16, 8, 8, 128), BF), pltpu.VMEM((128, 1024), BF),
                            pltpu.VMEM((4, 128, 256), BF), pltpu.VMEM((4, 128, 256), BF), pltpu.VMEM((16, 128, 256), BF),
                            pltpu.VMEM((256, 896), F32), pltpu.VMEM((128, 1), F32), pltpu.VMEM((16, 1, 128), F32),
                            pltpu.VMEM((4, 4, 32, 896), BF), pltpu.VMEM((128, 1024), F32),
                            pltpu.VMEM((4, 4, 32, 256), BF), pltpu.VMEM((4, 4, 32, 256), BF),
                            dma((12,)), dma((16,)), dma((16,)), dma((15,)), dma((16,)), dma((3,)), dma((4,)), dma((15,)), dma((16,)),
                            dma((4, 3)), dma((4, 4)), dma((4, 3)), dma((4, 4))],
            compiler_params=pltpu.CompilerParams(collective_id=1, has_side_effects=True, vmem_limit_bytes=48 * MIB),
            name="mlp",
        )(o, hidden, mlp_gain, w_out, w_gate_up, w_down)
        return hidden, k_out, v_out

    return jax.shard_map(
        layer,
        mesh=mesh,
        in_specs=(hidden_spec, P(batch_axes), P(), P(), P(None, None, 'yz'), P(None, 'yz', None),
                  P(None, None, None, 'yz'), P(None, 'yz', None), cache_spec, cache_spec),
        out_specs=(hidden_spec, cache_spec, cache_spec),
        check_vma=False)
```

```python
import functools

import jax
import jax.numpy as jnp
from jax import lax
from jax.experimental import pallas as pl
from jax.experimental.pallas import tpu as pltpu
from jax.sharding import PartitionSpec as P

NORM_EPS = 1e-5
MESH = pl.DeviceIdType.MESH
BF = jnp.bfloat16
F32 = jnp.float32
MIB = 1024 * 1024
GROUP = 4
CHUNK = 1024


def at(z, x):
    return {"yz": z, "x": x}


def remote(src, dst, ssem, rsem, z, x):
    return pltpu.make_async_remote_copy(src_ref=src, dst_ref=dst, send_sem=ssem, recv_sem=rsem,
                                        device_id=at(z, x), device_id_type=MESH)


def group_barrier(z, x, between=None):
    sem = pltpu.get_barrier_semaphore()
    me = z * 4 + x

    def body(p, c):
        d = lax.rem(me + p, 16)
        pl.semaphore_signal(sem, inc=1, device_id=at(lax.div(d, 4), lax.rem(d, 4)), device_id_type=MESH)
        return c

    lax.fori_loop(1, 16, body, 0)
    if between is not None:
        between()
    pl.semaphore_wait(sem, 15)


def by_distance(z):
    a, b = lax.div(z, 2), lax.rem(z, 2)
    first = lax.div(z + 3, 4)
    n1 = first * (z - 1) + (1 - first)
    n2 = 2 + a * (1 - 2 * b)
    return n1, n2, 6 - z - n1 - n2


def gather(buf, slot, src, ssem, rsem, z, x, ready, consume):
    yx = lax.rem(x + 2, 4)
    cx = x + 1 - 2 * lax.rem(x, 2)
    cyx = lax.rem(cx + 2, 4)
    n1, n2 = 1 + lax.rem(z, 2), 3 * (1 - lax.div(z, 2))
    n3 = 6 - z - n1 - n2
    end = 1 - lax.div(z * (3 - z), 2)
    me = slot(z, x)
    started = []

    def send(src, s, zt, xt):
        cp = remote(src, buf.at[s], ssem.at[len(started)], rsem.at[s], zt, xt)
        cp.start()
        started.append(cp)

    def arrived(s):
        remote(buf.at[s], buf.at[s], ssem.at[0], rsem.at[s], z, x).wait_recv()

    def pass_on(zt, xt, *targets):
        s = slot(zt, xt)
        arrived(s)
        for t in targets:
            send(buf.at[s], s, z, t)

    def work(first, second, *late):
        for zt, xt in late:
            arrived(slot(zt, xt))
        consume(slot(*first), slot(*second))

    send(src, me, z, yx)
    send(src, me, end * n2 + (1 - end) * n1, x)
    send(src, me, n3, x)
    third = slot(end * z + (1 - end) * n1, x)
    third = remote(buf.at[third], buf.at[third], ssem.at[len(started)], rsem.at[third], end * n1 + (1 - end) * n3, x)
    started.append(third)
    pl.when(end == 1)(third.start)
    send(src, me, z, cx)
    pass_on(z, yx, cx)
    arrived(slot(n1, x))
    pl.when(end == 0)(third.start)
    for t in (yx, cx):
        send(buf.at[slot(n1, x)], slot(n1, x), z, t)
    ready()
    work((z, x), (z, yx))
    pass_on(n2, x, yx, cx)
    work((n1, x), (z, cx), (z, cx))
    pass_on(n3, x, yx, cx)
    work((n2, x), (z, cyx), (z, cyx))
    pass_on(n1, yx, cx)
    work((n3, x), (n1, cx), (n1, cx))
    pass_on(n2, yx, cx)
    work((n1, yx), (n2, cx), (n2, cx))
    work((n2, yx), (n3, cx), (n3, cx))
    pass_on(n3, yx, cx)
    work((n3, yx), (n1, cyx), (n1, cyx))
    work((n2, cyx), (n3, cyx), (n2, cyx), (n3, cyx))
    return started


def share_sums(h, stat, ssem, rsem, z, x):
    me = z * 4 + x
    rows = h.shape[0]
    hf = h.astype(F32)
    sums = jnp.broadcast_to(jnp.sum(hf * hf, axis=1, keepdims=True), (rows, 128))
    stat[me] = jnp.transpose(sums)[0:1, :]

    def peer(p):
        d = lax.rem(me + p, 16)
        return remote(stat.at[me], stat.at[me], ssem.at[p], rsem.at[me], lax.div(d, 4), lax.rem(d, 4))

    def start(p, c):
        peer(p).start()
        return c

    lax.fori_loop(1, 16, start, 0)


def scale_of(stat, ssem, rsem, z, x, width):
    me = z * 4 + x

    def finish(p, c):
        remote(stat.at[me], stat.at[me], ssem.at[p], rsem.at[me], z, x).wait_send()
        d = lax.rem(me + p, 16)
        remote(stat.at[d], stat.at[d], ssem.at[0], rsem.at[d], z, x).wait_recv()
        return c

    lax.fori_loop(1, 16, finish, 0)
    tot = functools.reduce(lambda u, v: u + v, [stat[i] for i in range(16)])
    r = lax.rsqrt(tot / width + NORM_EPS)
    return jnp.transpose(jnp.broadcast_to(r, (128, 128)))[:, 0:1]


def normed(hb, gain, g, r):
    w = hb.shape[2]
    return (hb[g].astype(F32) * r * gain[:, pl.ds(pl.multiple_of(g * w, w), w)].astype(F32)).astype(BF)


def qkv_kernel(h_hbm, gain_hbm, w_hbm, out_ref, h_ref, gain, hb, wbuf, acc, scale, stat, zloc, zbuf,
               wsem, ssem, rsem, ssem_s, rsem_s, ssem2, rsem2, ssem3, rsem3):
    z, x = lax.axis_index("yz"), lax.axis_index("x")
    me = z * 4 + x
    parts = [
        pltpu.make_async_copy(w_hbm.at[0, pl.ds(pl.multiple_of(x * 256, 256), 256), :], wbuf.at[pl.ds(0, 256), :], wsem.at[0]),
        pltpu.make_async_copy(w_hbm.at[0, pl.ds(1024, 64), :], wbuf.at[pl.ds(256, 64), :], wsem.at[1]),
        pltpu.make_async_copy(w_hbm.at[0, pl.ds(1024, 64), :], wbuf.at[pl.ds(320, 64), :], wsem.at[2]),
        pltpu.make_async_copy(gain_hbm, gain, wsem.at[3]),
    ]
    mine = pltpu.make_async_copy(h_hbm, h_ref, wsem.at[4])
    mine.start()
    for cp in parts:
        cp.start()
    acc[...] = jnp.zeros_like(acc)
    group_barrier(z, x, mine.wait)
    share_sums(h_ref[...], stat, ssem_s, rsem_s, z, x)
    hb[x * 4 + z] = h_ref[...]

    def ready():
        scale[...] = scale_of(stat, ssem_s, rsem_s, z, x, 4096)
        for cp in parts:
            cp.wait()

    def consume(*pair):
        u = jnp.concatenate([normed(hb, gain, g, scale[...]) for g in pair], axis=1)
        w = jnp.concatenate([wbuf[:, pl.ds(pl.multiple_of(g * 256, 256), 256)] for g in pair], axis=1)
        acc[...] += lax.dot_general(u, w, (((1,), (1,)), ((), ())), preferred_element_type=F32)

    sent = gather(hb, lambda zt, xt: xt * 4 + zt, h_ref, ssem, rsem, z, x, ready, consume)
    for d in range(16):
        zloc[d] = acc[d * 8:(d + 1) * 8, :].astype(BF)

    main, tail, near = pl.ds(0, 256), pl.ds(256, 128), by_distance(z)
    tails = [remote(zloc.at[zt * 4 + x, :, tail], zbuf.at[me, :, tail], ssem3.at[i], rsem3.at[z], zt, x)
             for i, zt in enumerate(near)]

    def peer(p):
        d = lax.rem(me + p, 16)
        return remote(zloc.at[d, :, main], zbuf.at[me, :, main], ssem2.at[p], rsem2.at[me], lax.div(d, 4), lax.rem(d, 4))

    def start(p, c):
        peer(p).start()
        return c

    def finish(p, c):
        peer(p).wait_send()
        d = lax.rem(me + p, 16)
        remote(zbuf.at[d, :, main], zbuf.at[d, :, main], ssem2.at[0], rsem2.at[d], z, x).wait_recv()
        return c

    lax.fori_loop(1, 16, start, 0)
    for cp in tails:
        cp.start()
    zbuf[me] = zloc[me]
    for cp in sent:
        cp.wait_send()
    lax.fori_loop(1, 16, finish, 0)
    for cp, zt in zip(tails, near):
        cp.wait_send()
        d = zt * 4 + x
        remote(zbuf.at[d, :, tail], zbuf.at[d, :, tail], ssem3.at[0], rsem3.at[zt], z, x).wait_recv()
    out_ref[...] = zbuf[...]


def attn_kernel(len_ref, z_ref, k_ref, v_ref, o_ref, ko_hbm, vo_hbm, zrow, orow, tiles, qrow, score, osem, tsem):
    rows, positions, hd = k_ref.shape[1:]
    x = lax.axis_index("x")

    def store(b, which):
        src, dst = ((k_ref, ko_hbm), (v_ref, vo_hbm))[which]
        return pltpu.make_async_copy(src.at[0, b], dst.at[0, b], osem.at[which, b])

    def first(b):
        return pl.multiple_of(lax.div(len_ref[b], 16) * 16, 16)

    def patch(b, which):
        dst = (ko_hbm, vo_hbm)[which]
        return pltpu.make_async_copy(tiles.at[which, b], dst.at[0, b, pl.ds(first(b), 16), :], tsem.at[which, b])

    def start(b, c):
        store(b, 0).start()
        store(b, 1).start()
        return c

    lax.fori_loop(0, rows, start, 0)
    lane = lax.broadcasted_iota(jnp.int32, (rows, hd), 1)
    for pair in range(2):
        base = 17 * pair
        even, odd = 8 * pair, 8 * pair + 4
        mains_e = [z_ref[even + i // 2, :, (i % 2) * hd:(i % 2 + 1) * hd].astype(F32) for i in range(8)]
        mains_o = [pltpu.roll(z_ref[odd + i // 2, :, (i % 2) * hd:(i % 2 + 1) * hd].astype(F32), hd // 2, 1) for i in range(8)]
        tail_e = z_ref[even + x, :, 2 * hd:3 * hd].astype(F32)
        tail_o = z_ref[odd + x, :, 2 * hd:3 * hd].astype(F32)
        heads = mains_e + [jnp.where(lane < hd // 2, tail_e, mains_o[0])]
        for i in range(8):
            heads.append(jnp.where(lane < hd // 2, mains_o[i], mains_o[i + 1] if i < 7 else tail_o))
        for i, v in enumerate(heads):
            zrow[:, base + i, :] = v
    heads = zrow.shape[1] - 2
    factor = hd ** -0.5 * 1.4426950408889634

    def updated(ref, b, row, pos):
        lo = first(b)
        tile = ref[0, b, pl.ds(lo, 16), :].astype(F32)
        hit = lax.broadcasted_iota(jnp.int32, (16, hd), 0) == pos - lo
        return jnp.where(hit, row, tile).astype(BF)

    def renew(b, c):
        tiles[0, b] = updated(k_ref, b, zrow[b, heads:heads + 1, :], len_ref[b])
        tiles[1, b] = updated(v_ref, b, zrow[b, heads + 1:heads + 2, :], len_ref[b])
        return c

    lax.fori_loop(0, rows, renew, 0)

    qrow[...] = jnp.zeros_like(qrow)
    lane_row = lax.broadcasted_iota(jnp.int32, (1, GROUP * heads), 1)
    nt = (((1,), (1,)), ((), ()))

    def one(g, c):
        b0 = g * GROUP
        ends = jnp.zeros((1, GROUP * heads), jnp.int32)
        for i in range(GROUP):
            qrow[i * heads:(i + 1) * heads, i * hd:(i + 1) * hd] = zrow[b0 + i, 0:heads, :].astype(BF)
            ends = jnp.where(lax.div(lane_row, heads) == i, len_ref[b0 + i], ends)
        q = qrow[...]
        k_new = jnp.concatenate([jnp.broadcast_to(zrow[b0 + i, heads:heads + 1, :], (8, hd)) for i in range(GROUP)], axis=1)
        s_new = lax.dot_general(k_new.astype(BF), q, nt, preferred_element_type=F32)[0:1, :]
        top = s_new
        for lo in range(0, positions, CHUNK):
            k = jnp.concatenate([k_ref[0, b0 + i, lo:lo + CHUNK, :] for i in range(GROUP)], axis=1)
            s = lax.dot_general(k, q, nt, preferred_element_type=F32)
            ids = lax.broadcasted_iota(jnp.int32, s.shape, 0) + lo
            s = jnp.where(ids < ends, s, -1e30)
            score[lo:lo + CHUNK, :] = s
            top = jnp.maximum(top, jnp.max(s, axis=0, keepdims=True))
        e_new = jnp.exp2((s_new - top) * factor)
        total = e_new
        for lo in range(0, positions, CHUNK):
            e = jnp.exp2((score[lo:lo + CHUNK, :] - top) * factor)
            score[lo:lo + CHUNK, :] = e
            total += jnp.sum(e, axis=0, keepdims=True)
        inv = 1.0 / total
        p_new = jnp.transpose(jnp.broadcast_to((e_new * inv).astype(BF).astype(F32), (GROUP * heads, GROUP * heads)))
        outs = [p_new[i * heads:(i + 1) * heads, 0:1] * zrow[b0 + i, heads + 1:heads + 2, :] for i in range(GROUP)]
        for lo in range(0, positions, CHUNK):
            p = jnp.transpose((score[lo:lo + CHUNK, :] * inv).astype(BF))
            for i in range(GROUP):
                outs[i] += jnp.dot(p[i * heads:(i + 1) * heads, :], v_ref[0, b0 + i, lo:lo + CHUNK, :], preferred_element_type=F32)
        for i in range(GROUP):
            orow[b0 + i] = outs[i]
        return c

    def fix(b):
        for which in range(2):
            store(b, which).wait()
            patch(b, which).start()

    def patches(b, c):
        fix(b)
        return c

    lax.fori_loop(0, rows // GROUP, one, 0)
    lax.fori_loop(0, rows, patches, 0)
    for h in range(heads):
        o_ref[h // 8, h % 8] = orow[:, h, :].astype(BF)

    def finish(b, c):
        for which in range(2):
            patch(b, which).wait()
        return c

    lax.fori_loop(0, rows, finish, 0)


def mlp_kernel(o_hbm, h_hbm, gain_hbm, wo_hbm, wg_hbm, wd_hbm, out_ref,
               o_ref, h_ref, gain, wo, wg, wd, spread, obuf, olhs, part, recv, hb, acc, scale, stat, mbuf, low, part2, recv2,
               wsem, ssem_s, rsem_s, ssem_o, rsem_o, ssem_p, rsem_p, ssem_h, rsem_h, ssem_m, rsem_m, ssem_q, rsem_q):
    z, x = lax.axis_index("yz"), lax.axis_index("x")
    cols = pl.ds(pl.multiple_of(x * 1024, 1024), 1024)
    tiles = wg.shape[0]
    depth = wg.shape[1]
    flat = wg_hbm.at[0].reshape(depth, wg_hbm.shape[3])
    small = [pltpu.make_async_copy(o_hbm, o_ref, wsem.at[2 + tiles]), pltpu.make_async_copy(h_hbm, h_ref, wsem.at[3 + tiles]),
             pltpu.make_async_copy(gain_hbm, gain, wsem.at[4 + tiles])]
    for cp in small:
        cp.start()
    loads = [pltpu.make_async_copy(wo_hbm.at[0, :, cols], wo, wsem.at[0])]
    for j in range(tiles):
        lanes = pl.ds(pl.multiple_of((x * tiles + j) * 128, 128), 128)
        loads.append(pltpu.make_async_copy(flat.at[:, lanes], wg.at[j], wsem.at[1 + j]))
    loads.append(pltpu.make_async_copy(wd_hbm.at[0, :, cols], wd, wsem.at[1 + tiles]))
    for cp in loads:
        cp.start()
    def settle():
        k_id = lax.broadcasted_iota(jnp.int32, (256, 1024), 0)
        c_id = lax.broadcasted_iota(jnp.int32, (256, 1024), 1)
        spread[...] = jnp.where(c_id == 2 * k_id + (c_id // 512) * 513, 1.0, 0.0).astype(BF)
        acc[...] = jnp.zeros_like(acc)
        for cp in small:
            cp.wait()

    group_barrier(z, x, settle)
    yx = lax.rem(x + 2, 4)
    cx = x + 1 - 2 * lax.rem(x, 2)
    cyx = lax.rem(cx + 2, 4)
    near = by_distance(z)

    sent = []
    mine = z * 4 + x
    places = [(z, yx)] + [(zt, xt) for zt in near for xt in (x, yx)]

    def o_send(src, s, zt, xt):
        cp = remote(src, obuf.at[s], ssem_o.at[len(sent)], rsem_o.at[s], zt, xt)
        cp.start()
        sent.append(cp)

    def o_arrived(zt, xt):
        s = zt * 4 + xt
        remote(obuf.at[s], obuf.at[s], ssem_o.at[0], rsem_o.at[s], z, x).wait_recv()

    for zt, xt in places:
        o_send(o_ref.at[zt], mine, zt, xt)
    o_send(o_ref.at[z], mine, z, cx)
    obuf[mine] = o_ref[z]
    for zt, xt in places:
        o_arrived(zt, xt)
        o_send(obuf.at[zt * 4 + xt], zt * 4 + xt, z, cx)
    for zt in (z, *near):
        o_arrived(zt, cx)
        o_arrived(zt, cyx)
    for h in range(8):
        olhs[:, h * 128:(h + 1) * 128] = obuf[:, h].reshape(128, 128)

    loads[0].wait()

    def block(zt):
        return pl.ds(pl.multiple_of(zt * 256, 256), 256)

    for n in range(4):
        lanes = slice(n * 256, (n + 1) * 256)
        low[:, lanes] = jnp.dot(olhs[...], wo[:, lanes], preferred_element_type=F32)
    for i, zt in enumerate(near):
        part[zt] = low[:, block(zt)].astype(BF)
        cp = remote(part.at[zt], recv.at[z], ssem_p.at[i], rsem_p.at[z], zt, x)
        cp.start()
        sent.append(cp)
    total = low[:, block(z)]
    for zt in near:
        remote(recv.at[zt], recv.at[zt], ssem_p.at[0], rsem_p.at[zt], z, x).wait_recv()
        total += recv[zt].astype(F32)
    own = x * 4 + z
    hb[own] = (h_ref[...].astype(F32) + total).astype(BF)
    share_sums(hb[own], stat, ssem_s, rsem_s, z, x)

    def ready():
        scale[...] = scale_of(stat, ssem_s, rsem_s, z, x, 4096)
        for j in range(tiles):
            loads[1 + j].wait()

    def consume(*pair):
        u = jnp.concatenate([normed(hb, gain, g, scale[...]) for g in pair], axis=0)
        wide = jnp.dot(u, spread[...], preferred_element_type=F32).astype(BF)
        rows, width = hb.shape[1], wide.shape[1] // 2
        lhs = [jnp.concatenate([wide[i * rows:(i + 1) * rows, :width], wide[i * rows:(i + 1) * rows, width:]], axis=0)
               for i in range(len(pair))]
        lhs = jnp.concatenate(lhs, axis=1)
        for j in range(0, tiles, 2):
            width = min(2, tiles - j)
            w = jnp.concatenate([
                jnp.concatenate([wg[j + i, pl.ds(pl.multiple_of(g * 512, 512), 512), :] for i in range(width)], axis=1)
                for g in pair], axis=0)
            acc[:, j * 128:(j + width) * 128] += jnp.dot(lhs, w, preferred_element_type=F32)

    sent += gather(hb, lambda zt, xt: xt * 4 + zt, hb.at[own], ssem_h, rsem_h, z, x, ready, consume)
    pieces, half = mbuf.shape[0], mbuf.shape[2]

    def m_send(f, xt, target, i):
        cp = remote(mbuf.at[f, xt], mbuf.at[f, xt], ssem_m.at[f, i], rsem_m.at[f, xt], z, target)
        cp.start()
        sent.append(cp)

    def m_arrived(f, xt):
        remote(mbuf.at[f, xt], mbuf.at[f, xt], ssem_m.at[f, 0], rsem_m.at[f, xt], z, x).wait_recv()

    for f in range(pieces):
        gate = acc[f * half:(f + 1) * half, :].astype(BF).astype(F32)
        up = acc[128 + f * half:128 + (f + 1) * half, :].astype(BF).astype(F32)
        mbuf[f, x] = (jax.nn.silu(gate) * up).astype(BF)
        m_send(f, x, yx, 0)
        m_send(f, x, cx, 1)
    loads[1 + tiles].wait()

    width = mbuf.shape[3]

    def down(lhs, xt, lanes):
        return jnp.dot(lhs, wd[pl.ds(pl.multiple_of(xt * width, 128), width), lanes], preferred_element_type=F32)

    for xt in (x, cx):
        if xt is cx:
            for f in range(pieces):
                m_arrived(f, cx)
        lhs = jnp.concatenate([mbuf[f, xt] for f in range(pieces)], axis=0)
        for n in range(4):
            lanes = slice(n * 256, (n + 1) * 256)
            new = down(lhs, xt, lanes)
            low[:, lanes] = new if xt is x else low[:, lanes] + new

    def m_pass(f):
        m_arrived(f, yx)
        m_send(f, yx, cx, 2)

    m_pass(0)
    for f in range(pieces):
        rows = slice(f * half, (f + 1) * half)
        if f + 1 < pieces:
            m_pass(f + 1)
        m_arrived(f, cyx)
        for n in range(4):
            lanes = slice(n * 256, (n + 1) * 256)
            low[rows, lanes] += down(mbuf[f, yx], yx, lanes) + down(mbuf[f, cyx], cyx, lanes)
        for i, zt in enumerate(near):
            part2[f, zt] = low[rows, block(zt)].astype(BF)
            cp = remote(part2.at[f, zt], recv2.at[f, z], ssem_q.at[f, i], rsem_q.at[f, z], zt, x)
            cp.start()
            sent.append(cp)
    for f in range(pieces):
        rows = slice(f * half, (f + 1) * half)
        total = low[rows, block(z)]
        for zt in near:
            remote(recv2.at[f, zt], recv2.at[f, zt], ssem_q.at[f, 0], rsem_q.at[f, zt], z, x).wait_recv()
            total += recv2[f, zt].astype(F32)
        out_ref[rows, :] = (hb[own, rows, :].astype(F32) + total).astype(BF)
    for cp in sent:
        cp.wait_send()


def solution(mesh):
    hidden_spec = P('replica', ('x', 'yz'))
    batch_axes = ('replica', 'yz', 'x')
    cache_spec = P(None, batch_axes, None, None)
    vmem = pl.BlockSpec(memory_space=pltpu.VMEM)
    smem = pl.BlockSpec(memory_space=pltpu.SMEM)
    hbm = pl.BlockSpec(memory_space=pltpu.HBM)
    dma, sd = pltpu.SemaphoreType.DMA, jax.ShapeDtypeStruct

    def layer(hidden, seq_lens, attn_gain, mlp_gain, w_qkv, w_out, w_gate_up, w_down, k_cache, v_cache):
        w_qkv_t = jnp.swapaxes(w_qkv, 1, 2)
        z_rows = pl.pallas_call(
            qkv_kernel,
            out_shape=sd((16, 8, 384), BF),
            in_specs=[hbm, hbm, hbm],
            out_specs=vmem,
            scratch_shapes=[pltpu.VMEM((128, 256), BF), pltpu.VMEM((1, 4096), BF), pltpu.VMEM((16, 128, 256), BF), pltpu.VMEM((384, 4096), BF), pltpu.VMEM((128, 384), F32),
                            pltpu.VMEM((128, 1), F32), pltpu.VMEM((16, 1, 128), F32),
                            pltpu.VMEM((16, 8, 384), BF), pltpu.VMEM((16, 8, 384), BF),
                            dma((5,)), dma((15,)), dma((16,)), dma((16,)), dma((16,)), dma((16,)), dma((16,)),
                            dma((3,)), dma((4,))],
            compiler_params=pltpu.CompilerParams(collective_id=0, has_side_effects=True, vmem_limit_bytes=46 * MIB),
            cost_estimate=pl.CostEstimate(flops=30_000_000_000, bytes_accessed=20_000_000, transcendentals=0),
            name="qkv",
        )(pltpu.with_memory_space_constraint(hidden, pltpu.HBM), pltpu.with_memory_space_constraint(attn_gain, pltpu.HBM), w_qkv_t)
        rows, positions, hd = k_cache.shape[1:]
        o, k_out, v_out = pl.pallas_call(
            attn_kernel,
            out_shape=(sd((4, 8, rows, hd), BF), sd(k_cache.shape, BF), sd(v_cache.shape, BF)),
            in_specs=[smem, vmem, vmem, vmem],
            out_specs=(vmem, hbm, hbm),
            scratch_shapes=[pltpu.VMEM((rows, 34, hd), F32), pltpu.VMEM((rows, 32, hd), F32),
                            pltpu.VMEM((2, rows, 16, hd), BF), pltpu.VMEM((GROUP * 32, GROUP * hd), BF),
                            pltpu.VMEM((positions, GROUP * 32), F32), dma((2, rows)), dma((2, rows))],
            compiler_params=pltpu.CompilerParams(vmem_limit_bytes=28 * MIB),
            name="attend",
        )(seq_lens, z_rows, k_cache, v_cache)
        hidden = pl.pallas_call(
            mlp_kernel,
            out_shape=sd(hidden.shape, BF),
            in_specs=[hbm] * 6,
            out_specs=vmem,
            scratch_shapes=[pltpu.VMEM((4, 8, 8, 128), BF), pltpu.VMEM((128, 256), BF), pltpu.VMEM((1, 4096), BF),
                            pltpu.VMEM((1024, 1024), BF), pltpu.VMEM((7, 8192, 128), BF), pltpu.VMEM((3584, 1024), BF),
                            pltpu.VMEM((256, 1024), BF), pltpu.VMEM((16, 8, 8, 128), BF), pltpu.VMEM((128, 1024), BF),
                            pltpu.VMEM((4, 128, 256), BF), pltpu.VMEM((4, 128, 256), BF), pltpu.VMEM((16, 128, 256), BF),
                            pltpu.VMEM((256, 896), F32), pltpu.VMEM((128, 1), F32), pltpu.VMEM((16, 1, 128), F32),
                            pltpu.VMEM((4, 4, 32, 896), BF), pltpu.VMEM((128, 1024), F32),
                            pltpu.VMEM((4, 4, 32, 256), BF), pltpu.VMEM((4, 4, 32, 256), BF),
                            dma((12,)), dma((16,)), dma((16,)), dma((15,)), dma((16,)), dma((3,)), dma((4,)), dma((15,)), dma((16,)),
                            dma((4, 3)), dma((4, 4)), dma((4, 3)), dma((4, 4))],
            compiler_params=pltpu.CompilerParams(collective_id=1, has_side_effects=True, vmem_limit_bytes=48 * MIB),
            name="mlp",
        )(o, hidden, mlp_gain, w_out, w_gate_up, w_down)
        return hidden, k_out, v_out

    return jax.shard_map(
        layer,
        mesh=mesh,
        in_specs=(hidden_spec, P(batch_axes), P(), P(), P(None, None, 'yz'), P(None, 'yz', None),
                  P(None, None, None, 'yz'), P(None, 'yz', None), cache_spec, cache_spec),
        out_specs=(hidden_spec, cache_spec, cache_spec),
        check_vma=False)
```
